768 devices in a mesh: ctx: 16 (over z_hi, y), head: 48 (over x, z_lo, core).
Axes of the slice: x: 4, y: 8, z: 12 (z_hi: 2, z_lo: 6; z = z_hi * 6 + z_lo), core: 2. Of those that a mesh axis runs over, the one named last changes fastest.
Arguments:
- queries: bfloat16 [2048, 18432], P('ctx', 'head'), may hold values from -10 to 10
- latent: bfloat16 [2048, 576], P('ctx'), may hold values from -10 to 10
- block_of: int32 [32], replicated, may hold values from 0 to 31, each once
- key_up: bfloat16 [96, 128, 512], P('head'), may hold values from -0.5 to 0.5
- value_up: bfloat16 [96, 512, 128], P('head'), may hold values from -0.25 to 0.25
- out_grad: bfloat16 [2048, 12288], P('ctx', 'head'), may hold values from -6 to 6
Outputs:
- attended: bfloat16 [2048, 12288], P('ctx', 'head')
- query_grad: bfloat16 [2048, 18432], P('ctx', 'head')
- latent_grad: float32 [2048, 576], P('ctx')
The draws below stay inside these ranges and needn't reach their ends.
Inputs may be any that keep to these rules, and one draw needn't show every extreme that they name: `block_of`: a permutation of the 32 blocks.
All inputs are finite; a program needn't handle non-finite values.
Results may differ from the reference program's by a relative error of at most 0.0099.
Values may be sent and summed in bfloat16 or wider, within the bound.
A program may use at most 64 MiB of HBM per device.

```python
import math
import jax
import jax.numpy as jnp
from jax import lax

LATENT = 512
ROPE = 64
NOPE = 128
VHEAD = 128
HEADS = 96
TOKENS = 2048
BLK = 64
BLOCKS = 32


def draw_queries(key, part):
    shape = (TOKENS, HEADS, NOPE + ROPE)
    base = jnp.clip(jax.random.normal(jax.random.fold_in(key, 1), shape, jnp.float32), -6.0, 6.0)
    return base.reshape(TOKENS, HEADS * (NOPE + ROPE)).astype(jnp.bfloat16)


def draw_latent(key, part):
    shape = (TOKENS, LATENT + ROPE)
    base = jnp.clip(jax.random.normal(jax.random.fold_in(key, 3), shape, jnp.float32), -6.0, 6.0)
    return base.astype(jnp.bfloat16)


def levels(rng, dims, pieces, smallest, top_value):
    def one(position, shards_of):
        draws = jax.random.uniform(jax.random.fold_in(jax.random.fold_in(rng, 6), position), (shards_of,), jnp.float32, smallest / len(pieces), top_value / len(pieces))
        return jnp.repeat(jnp.exp(draws), dims[position] // shards_of).reshape((-1,) + (1,) * (len(dims) - position - 1))

    level = one(*pieces[0])
    for cut in pieces[1:]:
        level = level * one(*cut)
    return level


def gaussian(key, dims, spread, bound, shards=(), held_as=jnp.bfloat16):
    factor_of = levels(key, dims, shards, -0.22, 0.18) if shards else 1.0
    result = jax.random.normal(key, dims, jnp.float32) * spread * factor_of
    return jnp.minimum(jnp.maximum(result, -bound), bound).astype(held_as)


def setup_inputs(seed: int = 0) -> dict:
    key_of = jax.random.split(jax.random.key(seed), 7)
    return {
        "queries": draw_queries(jax.random.fold_in(key_of[6], 71), 0),
        "latent": draw_latent(jax.random.fold_in(key_of[6], 71), 0),
        "block_of": jax.random.permutation(key_of[2], BLOCKS).astype(jnp.int32),
        "key_up": gaussian(key_of[3], (HEADS, NOPE, LATENT), NOPE ** -0.5, 0.5, ((0, 48),)),
        "value_up": gaussian(key_of[4], (HEADS, LATENT, VHEAD), LATENT ** -0.5, 0.25, ((0, 48),)),
        "out_grad": gaussian(key_of[5], (TOKENS, HEADS * VHEAD), 1.0, 6.0, ((0, 16), (1, 48))),
    }


def reference(queries, latent, block_of, key_up, value_up, out_grad):
    rows = jnp.arange(TOKENS, dtype=jnp.int32)
    positions = jnp.take(block_of, (rows // BLK).astype(jnp.int32)).astype(jnp.int32) * BLK + rows % BLK
    visible = positions[None, :] <= positions[:, None]
    score_scale = 1.0 / math.sqrt(NOPE + ROPE)
    latent_part = latent[:, :LATENT]
    query_heads = jnp.transpose(queries.reshape(TOKENS, HEADS, NOPE + ROPE), (1, 0, 2))
    grad_heads = jnp.transpose(out_grad.reshape(TOKENS, HEADS, VHEAD), (1, 0, 2))

    def one_head(total, inputs):
        query_one, up_key, up_value, grad_one = inputs
        q_latent = jnp.dot(query_one[:, :NOPE], up_key, preferred_element_type=jnp.float32).astype(jnp.bfloat16)
        q_joined = jnp.concatenate([q_latent, query_one[:, NOPE:]], axis=1)
        scores = jnp.dot(q_joined, latent.T, preferred_element_type=jnp.float32) * score_scale
        scores = jnp.where(visible, scores, -1e+30)
        row_max = lax.optimization_barrier(jnp.max(scores, axis=1, keepdims=True))
        expo = jnp.exp(scores - row_max)
        probs = expo / lax.optimization_barrier(jnp.sum(expo, axis=1, keepdims=True))
        probs_low = probs.astype(jnp.bfloat16)
        out_latent = jnp.dot(probs_low, latent_part, preferred_element_type=jnp.float32).astype(jnp.bfloat16)
        attended = jnp.dot(out_latent, up_value, preferred_element_type=jnp.float32).astype(jnp.bfloat16)
        grad_latent = jnp.dot(grad_one, up_value.T, preferred_element_type=jnp.float32).astype(jnp.bfloat16)
        grad_probs = jnp.dot(grad_latent, latent_part.T, preferred_element_type=jnp.float32)
        delta = lax.optimization_barrier(jnp.sum(probs * grad_probs, axis=1, keepdims=True))
        grad_scores = (probs * (grad_probs - delta) * score_scale).astype(jnp.bfloat16)
        grad_joined = jnp.dot(grad_scores, latent, preferred_element_type=jnp.float32)
        grad_nope = jnp.dot(grad_joined[:, :LATENT].astype(jnp.bfloat16), up_key.T, preferred_element_type=jnp.float32).astype(jnp.bfloat16)
        grad_query = jnp.concatenate([grad_nope, grad_joined[:, LATENT:].astype(jnp.bfloat16)], axis=1)
        grad_keys = jnp.dot(grad_scores.T, q_joined, preferred_element_type=jnp.float32)
        value_part = jnp.dot(probs_low.T, grad_latent, preferred_element_type=jnp.float32)
        grad_keys = grad_keys + jnp.pad(value_part, ((0, 0), (0, ROPE)))
        return (total + grad_keys, (attended, grad_query))
    start = jnp.zeros((TOKENS, LATENT + ROPE), jnp.float32)
    latent_grad, (attended, query_grad) = lax.scan(one_head, start, (query_heads, key_up, value_up, grad_heads))
    attended = jnp.transpose(attended, (1, 0, 2)).reshape(TOKENS, HEADS * VHEAD)
    query_grad = jnp.transpose(query_grad, (1, 0, 2)).reshape(TOKENS, HEADS * (NOPE + ROPE))
    return (attended, query_grad, latent_grad)
```

```python
import functools
import math

import jax
import jax.numpy as jnp
from jax import lax
from jax.experimental import pallas as pl
from jax.experimental.pallas import tpu as pltpu
from jax.sharding import PartitionSpec as P

MESH = pl.DeviceIdType.MESH
NX, NY, NZH, NZL, NC = 4, 8, 2, 6, 2
NS = NX * NC
NP = NZH * NY
SR = 16
BF = jnp.bfloat16
F32 = jnp.float32


class Place:
    def __init__(self):
        c = lax.axis_index("ctx")
        h = lax.axis_index("head")
        self.c, self.h = c, h
        self.zh, self.y = c // NY, lax.rem(c, NY)
        self.k = lax.rem(h, NC)
        self.zl = lax.rem(h // NC, NZL)
        self.x = h // (NC * NZL)

    def at(self, zh=None, y=None, x=None, zl=None, k=None):
        zh = self.zh if zh is None else zh
        y = self.y if y is None else y
        x = self.x if x is None else x
        zl = self.zl if zl is None else zl
        k = self.k if k is None else k
        return (zh * NY + y, (x * NZL + zl) * NC + k)

    def partner(self):
        return self.at(k=1 - self.k)

    def mirror(self):
        return self.at(zh=1 - self.zh, zl=NZL - 1 - self.zl)

    def y_peer(self, d):
        return self.at(y=lax.rem(self.y + d, NY))

    def x_peer(self, d, other=False):
        return self.at(x=lax.rem(self.x + d, NX), k=1 - self.k if other else self.k)

    def zl_peer(self, d):
        return self.at(zl=lax.rem(self.zl + d, NZL))


def greet(peers):
    barrier = pltpu.get_barrier_semaphore()
    for peer in peers:
        pl.semaphore_signal(barrier, inc=1, device_id=peer, device_id_type=MESH)
    pl.semaphore_wait(barrier, len(peers))


def remote(src, dst, send_sem, recv_sem, peer):
    return pltpu.make_async_remote_copy(
        src_ref=src, dst_ref=dst, send_sem=send_sem, recv_sem=recv_sem,
        device_id=peer, device_id_type=MESH,
    )


Y_ORDER = (4, 3, 5, 2, 6, 1, 7)
X_ORDER = (2, 1, 3)


def gather_kernel(lat, out, ysend, yrecv, msend, mrecv, xsend, xrecv, dsend, drecv):
    me = Place()
    greet(
        [me.partner(), me.mirror()]
        + [me.y_peer(d) for d in range(1, NY)]
        + [me.x_peer(d) for d in range(1, NX)]
    )
    s = me.k * NX + me.x
    mine = lat.at[s]
    to_mirror = remote(mine, out.at[s, me.c], msend, mrecv, me.mirror())
    to_mirror.start()
    first = []
    for d in Y_ORDER:
        copy = remote(mine, out.at[s, me.c], ysend.at[0, d - 1], yrecv.at[0, d - 1], me.y_peer(d))
        copy.start()
        first.append(copy)
    out[s, me.c] = lat[s]
    far = 1 - me.zh

    to_mirror.wait()
    second = []
    got = out.at[s, far * NY + me.y]
    for d in Y_ORDER:
        copy = remote(got, got, ysend.at[1, d - 1], yrecv.at[1, d - 1], me.y_peer(d))
        copy.start()
        second.append(copy)

    def spread(group, half):
        part = out.at[s, pl.ds(half * NY, NY)]
        copies = []
        for d in X_ORDER:
            copy = remote(part, part, xsend.at[group, d - 1], xrecv.at[group, d - 1], me.x_peer(d))
            copy.start()
            copies.append(copy)
        cross = remote(part, part, dsend.at[group, 0], drecv.at[group, 0], me.partner())
        cross.start()
        return copies, [cross]

    def relay(group, half, copies, crosses):
        for d, copy in zip(X_ORDER, copies):
            copy.wait()
            source = me.k * NX + lax.rem(me.x + NX - d, NX)
            part = out.at[source, pl.ds(half * NY, NY)]
            cross = remote(part, part, dsend.at[group, d], drecv.at[group, d], me.partner())
            cross.start()
            crosses.append(cross)

    for copy in first:
        copy.wait()
    near_x, near_d = spread(0, me.zh)
    for copy in second:
        copy.wait()
    far_x, far_d = spread(1, far)
    relay(0, me.zh, near_x, near_d)
    relay(1, far, far_x, far_d)
    for cross in near_d + far_d:
        cross.wait()


def gather(latent):
    width = latent.shape[1]
    return pl.pallas_call(
        gather_kernel,
        out_shape=jax.ShapeDtypeStruct((NS, NP, SR, width), BF),
        in_specs=[pl.BlockSpec(memory_space=pltpu.VMEM)],
        out_specs=pl.BlockSpec(memory_space=pltpu.VMEM),
        scratch_shapes=[
            pltpu.SemaphoreType.DMA((2, NY - 1)),
            pltpu.SemaphoreType.DMA((2, NY - 1)),
            pltpu.SemaphoreType.DMA,
            pltpu.SemaphoreType.DMA,
            pltpu.SemaphoreType.DMA((2, NX - 1)),
            pltpu.SemaphoreType.DMA((2, NX - 1)),
            pltpu.SemaphoreType.DMA((2, NX)),
            pltpu.SemaphoreType.DMA((2, NX)),
        ],
        compiler_params=pltpu.CompilerParams(collective_id=0, has_side_effects=True),
    )(latent.reshape(NS, SR, width))


NT = (((1,), (1,)), ((), ()))
TN = (((0,), (0,)), ((), ()))
KC = 512


def attention_kernel(
    scale, q_ref, g_ref, ku_ref, vu_ref, lat_ref, kpos_ref, qpos_ref, att_ref, qg_ref, kt_ref,
    qr_ref, ql_ref, gl_ref, s_ref, gp_ref,
):
    heads, nope, width = ku_ref.shape
    value = vu_ref.shape[2]
    rows = q_ref.shape[0]
    keys = lat_ref.shape[0]
    rope = lat_ref.shape[1] - width
    head_width = nope + rope
    chunks = [pl.ds(i * KC, KC) for i in range(keys // KC)]
    for h in range(heads):
        at = pl.ds(h * rows, rows)
        qn = q_ref[:, h * head_width : h * head_width + nope]
        ql_ref[at, :] = jnp.dot(qn, ku_ref[h], preferred_element_type=F32).astype(BF)
        qr_ref[at, :] = q_ref[:, h * head_width + nope : (h + 1) * head_width]
        gl_ref[at, :] = lax.dot_general(
            g_ref[:, h * value : (h + 1) * value], vu_ref[h], NT, preferred_element_type=F32
        ).astype(BF)
    low = jnp.full((heads * rows, 1), -1e30, F32)
    for at in chunks:
        part = lax.dot_general(
            ql_ref[...], lat_ref[at, :width], NT, preferred_element_type=F32
        ) + lax.dot_general(qr_ref[...], lat_ref[at, width:], NT, preferred_element_type=F32)
        seen = kpos_ref[:, at] <= qpos_ref[...]
        part = part * scale
        for h in range(heads):
            s_ref[pl.ds(h * rows, rows), at] = jnp.where(
                seen, part[h * rows : (h + 1) * rows], -1e30
            )
        low = jnp.maximum(low, jnp.max(s_ref[:, at], axis=1, keepdims=True))
        gp_ref[:, at] = lax.dot_general(
            gl_ref[...], lat_ref[at, :width], NT, preferred_element_type=F32
        )
    total = jnp.zeros((heads * rows, 1), F32)
    delta = jnp.zeros((heads * rows, 1), F32)
    for at in chunks:
        expo = jnp.exp(s_ref[:, at] - low)
        s_ref[:, at] = expo
        total += jnp.sum(expo, axis=1, keepdims=True)
        delta += jnp.sum(expo * gp_ref[:, at], axis=1, keepdims=True)
    inverse = 1.0 / total
    delta = delta * inverse
    out = jnp.zeros((heads * rows, width), F32)
    joined = jnp.zeros((heads * rows, width), F32)
    joined_rope = jnp.zeros((heads * rows, rope), F32)
    for at in chunks:
        probs = s_ref[:, at] * inverse
        probs_low = probs.astype(BF)
        grads = (probs * (gp_ref[:, at] - delta) * scale).astype(BF)
        out += jnp.dot(probs_low, lat_ref[at, :width], preferred_element_type=F32)
        joined += jnp.dot(grads, lat_ref[at, :width], preferred_element_type=F32)
        joined_rope += jnp.dot(grads, lat_ref[at, width:], preferred_element_type=F32)
        kt_ref[at, :width] = (
            lax.dot_general(grads, ql_ref[...], TN, preferred_element_type=F32)
            + lax.dot_general(probs_low, gl_ref[...], TN, preferred_element_type=F32)
        ).astype(BF)
        kt_ref[at, width:] = lax.dot_general(
            grads, qr_ref[...], TN, preferred_element_type=F32
        ).astype(BF)
    for h in range(heads):
        part = slice(h * rows, (h + 1) * rows)
        att_ref[:, h * value : (h + 1) * value] = jnp.dot(
            out[part].astype(BF), vu_ref[h], preferred_element_type=F32
        ).astype(BF)
        qg_ref[:, h * head_width : h * head_width + nope] = lax.dot_general(
            joined[part].astype(BF), ku_ref[h], NT, preferred_element_type=F32
        ).astype(BF)
        qg_ref[:, h * head_width + nope : (h + 1) * head_width] = joined_rope[part].astype(BF)


def attention(scale, queries, out_grad, key_up, value_up, all_latent, key_pos, my_pos):
    rows = queries.shape[0]
    heads, nope, width = key_up.shape
    keys, joined = all_latent.shape
    both = heads * rows
    vmem = pl.BlockSpec(memory_space=pltpu.VMEM)
    return pl.pallas_call(
        functools.partial(attention_kernel, scale),
        out_shape=(
            jax.ShapeDtypeStruct(out_grad.shape, BF),
            jax.ShapeDtypeStruct(queries.shape, BF),
            jax.ShapeDtypeStruct((keys, joined), BF),
        ),
        in_specs=[vmem] * 7,
        out_specs=(vmem,) * 3,
        scratch_shapes=[
            pltpu.VMEM((both, joined - width), BF),
            pltpu.VMEM((both, width), BF),
            pltpu.VMEM((both, width), BF),
            pltpu.VMEM((both, keys), F32),
            pltpu.VMEM((both, keys), F32),
        ],
        compiler_params=pltpu.CompilerParams(vmem_limit_bytes=40 * 1024 * 1024),
        cost_estimate=pl.CostEstimate(
            flops=2 * both * keys * (6 * width), bytes_accessed=8 << 20, transcendentals=both * keys
        ),
    )(queries, out_grad, key_up, value_up, all_latent, key_pos, my_pos)


def reduce_kernel(
    terms, out, pair_in, x_out, x_in, y_out, y_in, m_out, m_in, z_in,
    dsend, drecv, xsend, xrecv, ysend, yrecv, msend, mrecv, zsend, zrecv, osend, orecv,
):
    me = Place()
    greet(
        [me.partner(), me.mirror()]
        + [me.y_peer(d) for d in range(1, NY)]
        + [me.x_peer(d) for d in range(1, NX)]
        + [me.x_peer(d, True) for d in range(1, NX)]
        + [me.zl_peer(d) for d in range(1, NZL)]
    )
    pairs = {}
    for d in X_ORDER + (0,):
        x = lax.rem(me.x + d, NX)
        copy = remote(terms.at[1 - me.k, x], pair_in.at[d], dsend.at[d], drecv.at[d], me.partner())
        copy.start()
        pairs[d] = copy
    moves = []
    for d in X_ORDER:
        x = lax.rem(me.x + d, NX)
        pairs[d].wait()
        x_out[d - 1] = (terms[me.k, x].astype(F32) + pair_in[d].astype(F32)).astype(BF)
        copy = remote(x_out.at[d - 1], x_in.at[d - 1], xsend.at[d - 1], xrecv.at[d - 1], me.x_peer(d))
        copy.start()
        moves.append(copy)
    pairs[0].wait()
    for copy in moves:
        copy.wait()
    for d in range(NY):
        y = lax.rem(me.y + d, NY)
        part = terms[me.k, me.x, :, y].astype(F32) + pair_in[0, :, y].astype(F32)
        for i in range(NX - 1):
            part += x_in[i, :, y].astype(F32)
        y_out[d] = part.astype(BF)
    moves = []
    for d in Y_ORDER:
        copy = remote(y_out.at[d], y_in.at[d - 1], ysend.at[d - 1], yrecv.at[d - 1], me.y_peer(d))
        copy.start()
        moves.append(copy)
    for copy in moves:
        copy.wait()

    def of_half(zh):
        part = y_out[0, zh].astype(F32)
        for i in range(NY - 1):
            part += y_in[i, zh].astype(F32)
        return part

    m_out[...] = of_half(1 - me.zh).astype(BF)
    to_mirror = remote(m_out, m_in, msend, mrecv, me.mirror())
    to_mirror.start()
    own = of_half(me.zh)
    to_mirror.wait()
    z_in[me.zl] = (own + m_in[...].astype(F32)).astype(BF)
    moves = []
    for d in (3, 2, 4, 1, 5):
        copy = remote(
            z_in.at[me.zl], z_in.at[me.zl], zsend.at[d - 1], zrecv.at[d - 1], me.zl_peer(d)
        )
        copy.start()
        moves.append(copy)
    for copy in moves:
        copy.wait()
    part = z_in[0].astype(F32)
    for i in range(1, NZL):
        part += z_in[i].astype(F32)
    s = me.k * NX + me.x
    out[s] = part.astype(BF)
    moves = []
    for j, peer in enumerate(
        [me.x_peer(d) for d in X_ORDER] + [me.x_peer(d, True) for d in X_ORDER] + [me.partner()]
    ):
        copy = remote(out.at[s], out.at[s], osend.at[j], orecv.at[j], peer)
        copy.start()
        moves.append(copy)
    for copy in moves:
        copy.wait()


def reduction(terms):
    width = terms.shape[-1]
    vmem = pl.BlockSpec(memory_space=pltpu.VMEM)
    dma = pltpu.SemaphoreType.DMA
    region = (NZH, NY, SR, width)
    return pl.pallas_call(
        reduce_kernel,
        out_shape=jax.ShapeDtypeStruct((NS, SR, width), BF),
        in_specs=[vmem],
        out_specs=vmem,
        scratch_shapes=[
            pltpu.VMEM((NX, *region), BF),
            pltpu.VMEM((NX - 1, *region), BF),
            pltpu.VMEM((NX - 1, *region), BF),
            pltpu.VMEM((NY, NZH, SR, width), BF),
            pltpu.VMEM((NY - 1, NZH, SR, width), BF),
            pltpu.VMEM((SR, width), BF),
            pltpu.VMEM((SR, width), BF),
            pltpu.VMEM((NZL, SR, width), BF),
            dma((NX,)), dma((NX,)),
            dma((NX - 1,)), dma((NX - 1,)),
            dma((NY - 1,)), dma((NY - 1,)),
            dma, dma,
            dma((NZL - 1,)), dma((NZL - 1,)),
            dma((7,)), dma((7,)),
        ],
        compiler_params=pltpu.CompilerParams(collective_id=1, has_side_effects=True),
    )(terms.reshape(NC, NX, *region))


def on_device(queries, latent, block_of, key_up, value_up, out_grad):
    rows, joined = latent.shape
    nope, width = key_up.shape[1:]
    scale = 1.0 / math.sqrt(nope + joined - width)
    block = rows // 2
    per_block = block // SR
    all_latent = gather(latent).reshape(NP * rows, joined)
    starts = jnp.transpose(block_of.reshape(NP, 2)) * block
    key_pos = (
        starts[:, None, :, None]
        + (jnp.arange(per_block, dtype=jnp.int32) * SR)[None, :, None, None]
        + jnp.arange(SR, dtype=jnp.int32)[None, None, None, :]
    ).reshape(1, NP * rows)
    mine = lax.dynamic_slice_in_dim(block_of, lax.axis_index("ctx") * 2, 2) * block
    my_pos = (mine[:, None] + jnp.arange(block, dtype=jnp.int32)[None, :]).reshape(rows, 1)
    attended, query_grad, terms = attention(
        scale, queries, out_grad, key_up, value_up, all_latent, key_pos, my_pos
    )
    latent_grad = reduction(terms).reshape(rows, joined).astype(F32)
    return attended, query_grad, latent_grad


def solution(mesh):
    return jax.shard_map(
        on_device,
        mesh=mesh,
        in_specs=(
            P("ctx", "head"),
            P("ctx", None),
            P(),
            P("head", None, None),
            P("head", None, None),
            P("ctx", "head"),
        ),
        out_specs=(P("ctx", "head"), P("ctx", "head"), P("ctx", None)),
        check_vma=False,
    )
```

```python
import functools
import math

import jax
import jax.numpy as jnp
from jax import lax
from jax.experimental import pallas as pl
from jax.experimental.pallas import tpu as pltpu
from jax.sharding import PartitionSpec as P

MESH = pl.DeviceIdType.MESH
NX, NY, NZH, NZL, NC = 4, 8, 2, 6, 2
SR = 16
LANES = 128
SLOTS = (0, 1, 7, 2, 6, 3, 5, 4)
SLOT_OF = {j: i for i, j in enumerate(SLOTS)}
HALF = NY // 2
GROUPS = (pl.ds(0, HALF), pl.ds(HALF, HALF))
TILE_OF = ((0, 1, 5, 6), (2, 3, 7, 8))
ROTARY_TILE = 4
TILES = 9
WIDE, NARROW = 5, 4
BF = jnp.bfloat16
F32 = jnp.float32
NT = (((1,), (1,)), ((), ()))
TN = (((0,), (0,)), ((), ()))


class Place:
    def __init__(self):
        self.c = lax.axis_index("ctx")
        h = lax.axis_index("head")
        self.zh, self.y = self.c // NY, lax.rem(self.c, NY)
        self.k = lax.rem(h, NC)
        self.zl = lax.rem(h // NC, NZL)
        self.x = h // (NC * NZL)
        self.odd = lax.rem(self.zl, 2)

    def at(self, dy=0, dx=0, dk=0, pair=0, dzl=0, far=0, mirror=False):
        zh = 1 - self.zh if far else self.zh
        y = lax.rem(self.y + dy, NY)
        x = lax.rem(self.x + dx, NX)
        k = 1 - self.k if dk else self.k
        zl = self.zl
        if mirror:
            zl = NZL - 1 - zl
        if pair:
            zl = zl + 1 - 2 * self.odd
        if dzl:
            zl = lax.rem(zl + dzl, NZL)
        return (zh * NY + y, (x * NZL + zl) * NC + k)


def kernel(
    scale, nope, rope, width, value, heads,
    blocks, lat, q_ref, g_ref, ku_ref, vu_ref,
    att_ref, qg_ref, grad_ref,
    keys, qr_ref, ql_ref, gl_ref, s_ref, gp_ref, p_ref, gs_ref,
    terms, pair_in, x_out, relay_in, direct_in, relay_out, sum_in,
    y_far, y_near, y_far_in, y_near_in, w_ref, z_own, z_out, z_far, final,
    y_send, y_recv, m_send, m_recv, x_send, x_recv, d_send, d_recv,
    p_send, p_recv, rx_send, rx_recv, ry_send, ry_recv, rz_send, rz_recv, f_send, f_recv,
):
    me = Place()
    rows = q_ref.shape[0]
    both = heads * rows
    head_width = nope + rope
    chunk = NC * NY * SR
    pending = []

    def send(src, dst, send_sem, recv_sem, peer):
        copy = pltpu.make_async_remote_copy(
            src_ref=src, dst_ref=dst, send_sem=send_sem, recv_sem=recv_sem,
            device_id=peer, device_id_type=MESH,
        )
        copy.start()
        pending.append(copy)
        return copy

    finals = [
        dict(pair=pair, dk=dk, dx=dx)
        for pair in range(2) for dk in range(NC) for dx in range(NX) if pair or dk or dx
    ]
    peers = (
        [dict(dy=d) for d in range(1, NY)]
        + [dict(dy=d, pair=1) for d in range(1, NY)]
        + finals
        + [dict(dzl=2), dict(dzl=4), dict(far=1), dict(far=1, dzl=2), dict(far=1, dzl=4)]
        + [dict(far=1, mirror=True)]
    )
    barrier = pltpu.get_barrier_semaphore()
    for peer in peers:
        pl.semaphore_signal(barrier, inc=1, device_id=me.at(**peer), device_id_type=MESH)

    for h in range(heads):
        at = pl.ds(h * rows, rows)
        qn = q_ref[:, h * head_width : h * head_width + nope]
        ql_ref[at, :] = jnp.dot(qn, ku_ref[h], preferred_element_type=F32).astype(BF)
        qr_ref[at, :] = q_ref[:, h * head_width + nope : (h + 1) * head_width]
        gl_ref[at, :] = lax.dot_general(
            g_ref[:, h * value : (h + 1) * value], vu_ref[h], NT, preferred_element_type=F32
        ).astype(BF)
    block = rows // 2
    row = lax.broadcasted_iota(jnp.int32, (rows, 1), 0)
    my_pos = jnp.where(row < block, blocks[2 * me.c], blocks[2 * me.c + 1]) * block + lax.rem(
        row, block
    )
    lane = lax.broadcasted_iota(jnp.int32, (1, chunk), 1)
    starts = []
    for zr in range(NZH):
        start = jnp.zeros((1, chunk), jnp.int32)
        for kr in range(NC):
            for slot, j in enumerate(SLOTS):
                zh = 1 - me.zh if zr else me.zh
                k = 1 - me.k if kr else me.k
                owner = zh * NY + lax.rem(me.y + j, NY)
                start = jnp.where(
                    lane // SR == kr * NY + slot, blocks[2 * owner + k] * block, start
                )
        starts.append(start + lax.rem(lane, SR))
    mine = pl.ds(pl.multiple_of((me.k * NX + me.x) * SR, SR), SR)
    keys[0, 0, 0, 0] = lat[mine, :]

    pl.semaphore_wait(barrier, len(peers))

    own = lat.at[mine, :]
    to_mirror = send(own, keys.at[1, 0, 0, 0], m_send, m_recv, me.at(far=1, mirror=True))

    def along_y(zr, src):
        return {
            NY - d: send(
                src, keys.at[zr, 0, 0, SLOT_OF[NY - d]],
                y_send.at[zr, d - 1], y_recv.at[zr, d - 1], me.at(dy=d),
            )
            for d in (7, 1, 6, 2, 5, 3, 4)
        }

    def x_copy(zr, i, src_x, dst_x, group, dx):
        return send(
            keys.at[zr, src_x, 0, GROUPS[group]], keys.at[zr, dst_x, 0, GROUPS[group]],
            x_send.at[zr, i], x_recv.at[zr, i], me.at(dx=dx),
        )

    def cross(zr, xr):
        return send(
            keys.at[zr, xr, 0], keys.at[zr, xr, 1], d_send.at[zr, xr], d_recv.at[zr, xr],
            me.at(dk=1),
        )

    def spread(zr, arrivals):
        for j in SLOTS[1:HALF]:
            arrivals[j].wait_recv()
        a_right = x_copy(zr, 0, 0, 3, 0, 1)
        a_left = x_copy(zr, 1, 0, 1, 0, 3)
        for j in SLOTS[HALF:]:
            arrivals[j].wait_recv()
        b_left = x_copy(zr, 2, 0, 1, 1, 3)
        b_right = x_copy(zr, 3, 0, 3, 1, 1)
        return a_right, a_left, b_left, b_right, cross(zr, 0)

    def forward(zr, moves):
        a_right, a_left, b_left, b_right, _ = moves
        a_right.wait_recv()
        relay_a = x_copy(zr, 4, 3, 2, 0, 1)
        b_left.wait_recv()
        relay_b = x_copy(zr, 5, 1, 2, 1, 3)
        b_right.wait_recv()
        from_left = cross(zr, 3)
        a_left.wait_recv()
        from_right = cross(zr, 1)
        return relay_a, relay_b, from_left, from_right

    def close(zr, relays):
        relays[0].wait_recv()
        relays[1].wait_recv()
        return cross(zr, 2)

    maxima = []

    def score(zr, xr, arrived):
        arrived.wait_recv()
        at = pl.ds((zr * NX + xr) * chunk, chunk)
        k_val = keys[zr, xr].reshape(chunk, width + rope)
        part = lax.dot_general(
            ql_ref[...], k_val[:, :width], NT, preferred_element_type=F32
        ) + lax.dot_general(qr_ref[...], k_val[:, width:], NT, preferred_element_type=F32)
        key_pos = starts[zr] + lax.rem(me.x + xr, NX) * SR
        seen = key_pos <= my_pos
        part = part * scale
        part = jnp.concatenate(
            [jnp.where(seen, part[h * rows : (h + 1) * rows], -1e30) for h in range(heads)], axis=0
        )
        s_ref[:, at] = part
        maxima.append(jnp.max(part, axis=1, keepdims=True))
        gp_ref[:, at] = lax.dot_general(
            gl_ref[...], k_val[:, :width], NT, preferred_element_type=F32
        )

    near = along_y(0, own)
    near_moves = spread(0, near)
    to_mirror.wait_recv()
    far = along_y(1, keys.at[1, 0, 0, 0])
    near_relays = forward(0, near_moves)
    score(0, 0, near_moves[4])
    far_moves = spread(1, far)
    near_last = close(0, near_relays)
    score(0, 3, near_relays[2])
    score(0, 1, near_relays[3])
    far_relays = forward(1, far_moves)
    score(0, 2, near_last)
    score(1, 0, far_moves[4])
    far_last = close(1, far_relays)
    score(1, 3, far_relays[2])
    score(1, 1, far_relays[3])
    score(1, 2, far_last)

    low = functools.reduce(jnp.maximum, maxima)
    total = jnp.zeros((both, 1), F32)
    delta = jnp.zeros((both, 1), F32)
    for i in range(NZH * NX):
        at = pl.ds(i * chunk, chunk)
        expo = jnp.exp(s_ref[:, at] - low)
        s_ref[:, at] = expo
        total += jnp.sum(expo, axis=1, keepdims=True)
        delta += jnp.sum(expo * gp_ref[:, at], axis=1, keepdims=True)
    inverse = 1.0 / total
    delta = delta * inverse

    crossings = {}
    for xr in (2, 1, 3, 0):
        rotary = []
        for zr in range(NZH):
            at = pl.ds((zr * NX + xr) * chunk, chunk)
            probs = s_ref[:, at] * inverse
            probs_low = probs.astype(BF)
            grads = (probs * (gp_ref[:, at] - delta) * scale).astype(BF)
            p_ref[:, at] = probs_low
            gs_ref[:, at] = grads
            wide = lax.dot_general(
                grads, ql_ref[...], TN, preferred_element_type=F32
            ) + lax.dot_general(probs_low, gl_ref[...], TN, preferred_element_type=F32)
            rotary.append(lax.dot_general(grads, qr_ref[...], TN, preferred_element_type=F32))
            for kr in range(NC):
                part = wide[kr * NY * SR : (kr + 1) * NY * SR].astype(BF)
                for t in range(width // LANES):
                    terms[kr, xr, TILE_OF[zr][t]] = part[:, t * LANES : (t + 1) * LANES].reshape(
                        NY, SR, LANES
                    )
        for kr in range(NC):
            cut = slice(kr * NY * SR, (kr + 1) * NY * SR)
            terms[kr, xr, ROTARY_TILE] = (
                jnp.concatenate([r[cut] for r in rotary], axis=1).astype(BF).reshape(NY, SR, LANES)
            )
        crossings[xr] = send(
            terms.at[1, xr], pair_in.at[xr], p_send.at[xr], p_recv.at[xr], me.at(dk=1)
        )

    windows = (
        (pl.ds(4 * (1 - me.odd), WIDE), pl.ds(0, WIDE), WIDE),
        (pl.ds(5 * me.odd, NARROW), pl.ds(WIDE, NARROW), NARROW),
    )
    for xr in (2, 1, 3):
        crossings[xr].wait_recv()
        for t in range(TILES):
            x_out[xr - 1, t] = (
                terms[0, xr, t].astype(F32) + pair_in[xr, t].astype(F32)
            ).astype(BF)
        if xr == 2:
            hops = {}
            for w in (0,):
                src, dst, _ = windows[w]
                hops[w, 0] = send(
                    x_out.at[1, src, GROUPS[0]], relay_in.at[0, dst],
                    rx_send.at[w, 0], rx_recv.at[w, 0], me.at(dx=1),
                )
                hops[w, 1] = send(
                    x_out.at[1, src, GROUPS[1]], relay_in.at[1, dst],
                    rx_send.at[w, 1], rx_recv.at[w, 1], me.at(dx=3),
                )

    def direct(w):
        src, dst, _ = windows[w]
        hops[w, 2] = send(
            x_out.at[0, src, GROUPS[1]], direct_in.at[0, dst],
            rx_send.at[w, 2], rx_recv.at[w, 2], me.at(dx=1),
        )
        hops[w, 3] = send(
            x_out.at[2, src, GROUPS[0]], direct_in.at[1, dst],
            rx_send.at[w, 3], rx_recv.at[w, 3], me.at(dx=3),
        )

    def relayed(w):
        src, dst, count = windows[w]
        for side, (xi, dx) in enumerate(((0, 1), (2, 3))):
            hops[w, side].wait_recv()
            relay_out[side, dst] = (
                x_out[xi, src, GROUPS[side]].astype(F32) + relay_in[side, dst].astype(F32)
            ).astype(BF)
            hops[w, 4 + side] = send(
                relay_out.at[side, dst], sum_in.at[side, dst],
                rx_send.at[w, 4 + side], rx_recv.at[w, 4 + side], me.at(dx=dx),
            )

    direct(0)
    src, dst, _ = windows[1]
    hops[1, 0] = send(
        x_out.at[1, src, GROUPS[0]], relay_in.at[0, dst],
        rx_send.at[1, 0], rx_recv.at[1, 0], me.at(dx=1),
    )
    hops[1, 1] = send(
        x_out.at[1, src, GROUPS[1]], relay_in.at[1, dst],
        rx_send.at[1, 1], rx_recv.at[1, 1], me.at(dx=3),
    )
    crossings[0].wait_recv()

    out = jnp.zeros((both, width), F32)
    step = 2 * chunk
    for zr in range(NZH):
        for half in range(2):
            at = pl.ds((zr * NX + 2 * half) * chunk, step)
            k_val = keys[zr, 2 * half : 2 * half + 2].reshape(step, width + rope)
            out += jnp.dot(p_ref[:, at], k_val[:, :width], preferred_element_type=F32)
    for h in range(heads):
        part = slice(h * rows, (h + 1) * rows)
        att_ref[:, h * value : (h + 1) * value] = jnp.dot(
            out[part].astype(BF), vu_ref[h], preferred_element_type=F32
        ).astype(BF)
    relayed(0)
    direct(1)
    joined = jnp.zeros((both, width), F32)
    joined_rotary = jnp.zeros((both, rope), F32)
    for zr in range(NZH):
        for half in range(2):
            at = pl.ds((zr * NX + 2 * half) * chunk, step)
            k_val = keys[zr, 2 * half : 2 * half + 2].reshape(step, width + rope)
            joined += jnp.dot(gs_ref[:, at], k_val[:, :width], preferred_element_type=F32)
            joined_rotary += jnp.dot(gs_ref[:, at], k_val[:, width:], preferred_element_type=F32)
    for h in range(heads):
        part = slice(h * rows, (h + 1) * rows)
        qg_ref[:, h * head_width : h * head_width + nope] = lax.dot_general(
            joined[part].astype(BF), ku_ref[h], NT, preferred_element_type=F32
        ).astype(BF)
        qg_ref[:, h * head_width + nope : (h + 1) * head_width] = joined_rotary[part].astype(BF)
    relayed(1)

    def summed(w, i):
        src, dst, _ = windows[w]
        tile = src.start + i
        at = dst.start + i
        base = terms[0, 0, tile].astype(F32) + pair_in[0, tile].astype(F32)
        first = base[:HALF] + sum_in[0, at].astype(F32) + direct_in[1, at].astype(F32)
        second = base[HALF:] + direct_in[0, at].astype(F32) + sum_in[1, at].astype(F32)
        return jnp.concatenate([first, second], axis=0).astype(BF)

    for i in range(2, 6):
        hops[0, i].wait_recv()
    for i in range(WIDE):
        y_far[:, i] = summed(0, i)
    ups = [
        send(
            y_far.at[slot], y_far_in.at[slot], ry_send.at[0, slot], ry_recv.at[0, slot],
            me.at(dy=SLOTS[slot], pair=1),
        )
        for slot in reversed(range(NY))
    ]
    for i in range(2, 6):
        hops[1, i].wait_recv()
    for i in range(NARROW):
        y_near[:, me.odd + i] = summed(1, i)
    y_near[:, 4 * (1 - me.odd)] = y_far[:, 4 * me.odd]
    ups += [
        send(
            y_near.at[slot], y_near_in.at[slot - 1], ry_send.at[1, slot], ry_recv.at[1, slot],
            me.at(dy=SLOTS[slot]),
        )
        for slot in reversed(range(1, NY))
    ]
    for up in ups:
        up.wait_recv()
    part = y_near[0].astype(F32)
    for i in range(NY):
        part += y_far_in[i].astype(F32)
    for i in range(NY - 1):
        part += y_near_in[i].astype(F32)
    w_ref[...] = part

    order = me.zl // 2
    rotary = w_ref[4 * (1 - me.odd)]
    z_out[0:2] = w_ref[pl.ds(2 + me.odd, 2)].astype(BF)
    z_out[2] = jnp.concatenate([rotary[:, rope:], rotary[:, :rope]], axis=1).astype(BF)
    ups = [
        send(
            z_out, z_far.at[order], rz_send.at[2 + i], rz_recv.at[2 + i], me.at(far=1, dzl=2 * i)
        )
        for i in range(3)
    ]
    z_own[order, 0:2] = w_ref[pl.ds(me.odd, 2)].astype(BF)
    z_own[order, 2] = rotary.astype(BF)
    ups += [
        send(
            z_own.at[order], z_own.at[order], rz_send.at[i], rz_recv.at[i], me.at(dzl=2 * i + 2)
        )
        for i in range(2)
    ]
    for up in ups:
        up.wait_recv()
    part = z_own[0].astype(F32)
    for i in range(1, 3):
        part += z_own[i].astype(F32)
    for i in range(3):
        part += z_far[i].astype(F32)
    final[me.odd, me.k, me.x] = part.astype(BF)
    place = final.at[me.odd, me.k, me.x]
    ups = [
        send(place, place, f_send.at[i], f_recv.at[i], me.at(**peer))
        for i, peer in enumerate(finals)
    ]
    for up in ups:
        up.wait_recv()
    for odd in range(2):
        for t in range(2):
            column = (2 * odd + t) * LANES
            grad_ref[:, column : column + LANES] = (
                final[odd, :, :, t].reshape(NC * NX * SR, LANES).astype(F32)
            )
    grad_ref[:, width:] = final[0, :, :, 2].reshape(NC * NX * SR, LANES)[:, :rope].astype(F32)
    for copy in pending:
        copy.wait_send()


def on_device(queries, latent, block_of, key_up, value_up, out_grad):
    rows, joined = latent.shape
    heads, nope, width = key_up.shape
    value = value_up.shape[2]
    rope = joined - width
    scale = 1.0 / math.sqrt(nope + rope)
    both = heads * rows
    total = NZH * NX * NC * NY * SR
    vmem = pl.BlockSpec(memory_space=pltpu.VMEM)
    dma = pltpu.SemaphoreType.DMA
    tile = (SR, LANES)
    return pl.pallas_call(
        functools.partial(kernel, scale, nope, rope, width, value, heads),
        out_shape=(
            jax.ShapeDtypeStruct(out_grad.shape, BF),
            jax.ShapeDtypeStruct(queries.shape, BF),
            jax.ShapeDtypeStruct((rows, joined), F32),
        ),
        in_specs=[pl.BlockSpec(memory_space=pltpu.SMEM)] + [vmem] * 5,
        out_specs=(vmem,) * 3,
        scratch_shapes=[
            pltpu.VMEM((NZH, NX, NC, NY, SR, joined), BF),
            pltpu.VMEM((both, rope), BF),
            pltpu.VMEM((both, width), BF),
            pltpu.VMEM((both, width), BF),
            pltpu.VMEM((both, total), F32),
            pltpu.VMEM((both, total), F32),
            pltpu.VMEM((both, total), BF),
            pltpu.VMEM((both, total), BF),
            pltpu.VMEM((NC, NX, TILES, NY, *tile), BF),
            pltpu.VMEM((NX, TILES, NY, *tile), BF),
            pltpu.VMEM((NX - 1, TILES, NY, *tile), BF),
            pltpu.VMEM((2, TILES, HALF, *tile), BF),
            pltpu.VMEM((2, TILES, HALF, *tile), BF),
            pltpu.VMEM((2, TILES, HALF, *tile), BF),
            pltpu.VMEM((2, TILES, HALF, *tile), BF),
            pltpu.VMEM((NY, WIDE, *tile), BF),
            pltpu.VMEM((NY, WIDE, *tile), BF),
            pltpu.VMEM((NY, WIDE, *tile), BF),
            pltpu.VMEM((NY - 1, WIDE, *tile), BF),
            pltpu.VMEM((WIDE, *tile), F32),
            pltpu.VMEM((3, 3, *tile), BF),
            pltpu.VMEM((3, *tile), BF),
            pltpu.VMEM((3, 3, *tile), BF),
            pltpu.VMEM((2, NC, NX, 3, *tile), BF),
            dma((2, NY - 1)), dma((2, NY - 1)),
            dma, dma,
            dma((2, 6)), dma((2, 6)),
            dma((2, NX)), dma((2, NX)),
            dma((NX,)), dma((NX,)),
            dma((2, 6)), dma((2, 6)),
            dma((2, NY)), dma((2, NY)),
            dma((5,)), dma((5,)),
            dma((15,)), dma((15,)),
        ],
        compiler_params=pltpu.CompilerParams(
            collective_id=0, has_side_effects=True, vmem_limit_bytes=48 * 1024 * 1024
        ),
    )(block_of, latent, queries, out_grad, key_up, value_up)


def solution(mesh):
    return jax.shard_map(
        on_device,
        mesh=mesh,
        in_specs=(
            P("ctx", "head"),
            P("ctx", None),
            P(),
            P("head", None, None),
            P("head", None, None),
            P("ctx", "head"),
        ),
        out_specs=(P("ctx", "head"), P("ctx", "head"), P("ctx", None)),
        check_vma=False,
    )
```

```python
import functools
import math

import jax
import jax.numpy as jnp
from jax import lax
from jax.experimental import pallas as pl
from jax.experimental.pallas import tpu as pltpu
from jax.sharding import PartitionSpec as P

MESH = pl.DeviceIdType.MESH
NX, NY, NZH, NZL, NC = 4, 8, 2, 6, 2
SR = 16
LANES = 128
SLOTS = (0, 1, 7, 2, 6, 3, 5, 4)
SLOT_OF = {j: i for i, j in enumerate(SLOTS)}
HALF = NY // 2
GROUPS = (pl.ds(0, HALF), pl.ds(HALF, HALF))
TILE_OF = ((0, 1, 5, 6), (2, 3, 7, 8))
ROTARY_TILE = 4
TILES = 9
WIDE, NARROW = 5, 4
BF = jnp.bfloat16
F32 = jnp.float32
NT = (((1,), (1,)), ((), ()))
TN = (((0,), (0,)), ((), ()))


class Place:
    def __init__(self):
        self.c = lax.axis_index("ctx")
        h = lax.axis_index("head")
        self.zh, self.y = self.c // NY, lax.rem(self.c, NY)
        self.k = lax.rem(h, NC)
        self.zl = lax.rem(h // NC, NZL)
        self.x = h // (NC * NZL)
        self.odd = lax.rem(self.zl, 2)
        self.side = lax.rem(self.zl + self.zh, 2)

    def at(self, dy=0, dx=0, dk=0, pair=0, dzl=0, far=0, mirror=False):
        zh = 1 - self.zh if far else self.zh
        y = lax.rem(self.y + dy, NY)
        x = lax.rem(self.x + dx, NX)
        k = 1 - self.k if dk else self.k
        zl = self.zl
        if mirror:
            zl = NZL - 1 - zl
        if pair:
            zl = zl + 1 - 2 * self.odd
        if dzl:
            zl = lax.rem(zl + dzl, NZL)
        return (zh * NY + y, (x * NZL + zl) * NC + k)


def kernel(
    scale, nope, rope, width, value, heads,
    blocks, lat_hbm, q_hbm, g_hbm, ku_hbm, vu_hbm,
    att_ref, qg_ref, grad_ref,
    final, lat_t, lat, q_ref, g_ref, ku_ref, vu_ref, in_sem,
    keys, qr_ref, ql_ref, gl_ref, s_ref, gp_ref, p_ref, gs_ref,
    terms, pair_in, x_out, relay_in, direct_in, relay_out, sum_in,
    y_far, y_near, y_far_in, y_near_in, w_ref, z_own, z_out, z_far,
    y_send, y_recv, m_send, m_recv, x_send, x_recv, d_send, d_recv,
    p_send, p_recv, rx_send, rx_recv, ry_send, ry_recv, rz_send, rz_recv, f_send, f_recv,
):
    me = Place()
    rows = q_ref.shape[0]
    both = heads * rows
    head_width = nope + rope
    chunk = NC * NY * SR
    pending = []

    def send(src, dst, send_sem, recv_sem, peer):
        copy = pltpu.make_async_remote_copy(
            src_ref=src, dst_ref=dst, send_sem=send_sem, recv_sem=recv_sem,
            device_id=peer, device_id_type=MESH,
        )
        copy.start()
        pending.append(copy)
        return copy

    finals = [
        dict(pair=pair, dk=dk, dx=dx)
        for pair in range(2) for dk in range(NC) for dx in range(NX) if pair or dk or dx
    ]
    peers = (
        [dict(dy=d) for d in range(1, NY)]
        + [dict(dy=d, pair=1) for d in range(1, NY)]
        + finals
        + [dict(dzl=2), dict(dzl=4)]
        + [dict(far=1, mirror=True, dzl=d) for d in (0, 2, 4)]
    )
    barrier = pltpu.get_barrier_semaphore()
    for peer in peers:
        pl.semaphore_signal(barrier, inc=1, device_id=me.at(**peer), device_id_type=MESH)

    loads = [
        pltpu.make_async_copy(src, dst, in_sem.at[i])
        for i, (src, dst) in enumerate(
            ((lat_hbm, lat_t), (q_hbm, q_ref), (ku_hbm, ku_ref), (g_hbm, g_ref), (vu_hbm, vu_ref))
        )
    ]
    for load in loads:
        load.start()
    loads[0].wait()
    for t in range(0, width, LANES):
        lat[:, t : t + LANES] = lat_t[t : t + LANES, :].T
    lat[:, width:] = lat_t[width:, :].T
    for load in loads[1:]:
        load.wait()
    for h in range(heads):
        at = pl.ds(h * rows, rows)
        qn = q_ref[:, h * head_width : h * head_width + nope]
        ql_ref[at, :] = jnp.dot(qn, ku_ref[h], preferred_element_type=F32).astype(BF)
        qr_ref[at, :] = q_ref[:, h * head_width + nope : (h + 1) * head_width]
        gl_ref[at, :] = lax.dot_general(
            g_ref[:, h * value : (h + 1) * value], vu_ref[h], NT, preferred_element_type=F32
        ).astype(BF)
    block = rows // 2
    row = lax.broadcasted_iota(jnp.int32, (rows, 1), 0)
    my_pos = jnp.where(row < block, blocks[2 * me.c], blocks[2 * me.c + 1]) * block + lax.rem(
        row, block
    )
    lane = lax.broadcasted_iota(jnp.int32, (1, chunk), 1)
    starts = []
    for zr in range(NZH):
        start = jnp.zeros((1, chunk), jnp.int32)
        for kr in range(NC):
            for slot, j in enumerate(SLOTS):
                zh = 1 - me.zh if zr else me.zh
                k = 1 - me.k if kr else me.k
                owner = zh * NY + lax.rem(me.y + j, NY)
                start = jnp.where(
                    lane // SR == kr * NY + slot, blocks[2 * owner + k] * block, start
                )
        starts.append(start + lax.rem(lane, SR))
    mine = pl.ds(pl.multiple_of((me.k * NX + me.x) * SR, SR), SR)
    keys[0, 0, 0, 0] = lat[mine, :]

    pl.semaphore_wait(barrier, len(peers))

    own = lat.at[mine, :]
    to_mirror = send(own, keys.at[1, 0, 0, 0], m_send, m_recv, me.at(far=1, mirror=True))

    def along_y(zr, src):
        return {
            NY - d: send(
                src, keys.at[zr, 0, 0, SLOT_OF[NY - d]],
                y_send.at[zr, d - 1], y_recv.at[zr, d - 1], me.at(dy=d),
            )
            for d in (7, 1, 6, 2, 5, 3, 4)
        }

    def x_copy(zr, i, src_x, dst_x, part, dx):
        return send(
            keys.at[zr, src_x, 0, part], keys.at[zr, dst_x, 0, part],
            x_send.at[zr, i], x_recv.at[zr, i], me.at(dx=dx),
        )

    def cross(zr, xr):
        return send(
            keys.at[zr, xr, 0], keys.at[zr, xr, 1], d_send.at[zr, xr], d_recv.at[zr, xr],
            me.at(dk=1),
        )

    def spread(zr, group, arrivals):
        for j in SLOTS[group * HALF : (group + 1) * HALF]:
            if j:
                arrivals[j].wait_recv()
        part = GROUPS[group]
        return (
            x_copy(zr, 4 * group, 0, 3, part, 1),
            x_copy(zr, 4 * group + 1, 0, 1, part, 3),
        )

    def relay(zr, group, moves):
        start = group * HALF
        moves[0].wait_recv()
        right = x_copy(zr, 4 * group + 2, 3, 2, pl.ds(start, HALF // 2), 1)
        moves[1].wait_recv()
        left = x_copy(zr, 4 * group + 3, 1, 2, pl.ds(start + HALF // 2, HALF // 2), 3)
        return right, left

    def close(zr, *relays):
        for copy in relays:
            copy.wait_recv()
        return cross(zr, 2)

    stats = {}

    def score(zr, xr, arrived):
        arrived.wait_recv()
        at = pl.ds((zr * NX + xr) * chunk, chunk)
        k_val = keys[zr, xr].reshape(chunk, width + rope)
        part = lax.dot_general(
            ql_ref[...], k_val[:, :width], NT, preferred_element_type=F32
        ) + lax.dot_general(qr_ref[...], k_val[:, width:], NT, preferred_element_type=F32)
        key_pos = starts[zr] + lax.rem(me.x + xr, NX) * SR
        seen = key_pos <= my_pos
        part = part * scale
        part = jnp.concatenate(
            [jnp.where(seen, part[h * rows : (h + 1) * rows], -1e30) for h in range(heads)], axis=0
        )
        high = jnp.max(part, axis=1, keepdims=True)
        expo = jnp.exp(part - high)
        back = lax.dot_general(gl_ref[...], k_val[:, :width], NT, preferred_element_type=F32)
        s_ref[:, at] = expo
        gp_ref[:, at] = back
        stats[zr, xr] = (
            high,
            jnp.sum(expo, axis=1, keepdims=True),
            jnp.sum(expo * back, axis=1, keepdims=True),
        )

    near = along_y(0, own)
    near_a = spread(0, 0, near)
    to_mirror.wait_recv()
    far = along_y(1, keys.at[1, 0, 0, 0])
    near_b = spread(0, 1, near)
    across = {(0, 0): cross(0, 0)}
    near_relay_a = relay(0, 0, near_a)
    far_a = spread(1, 0, far)
    near_relay_b = relay(0, 1, near_b)
    across[0, 3] = cross(0, 3)
    across[0, 1] = cross(0, 1)
    score(0, 0, across[0, 0])
    far_b = spread(1, 1, far)
    across[1, 0] = cross(1, 0)
    across[0, 2] = close(0, *near_relay_a, *near_relay_b)
    far_relay_a = relay(1, 0, far_a)
    score(0, 3, across[0, 3])
    score(0, 1, across[0, 1])
    far_relay_b = relay(1, 1, far_b)
    across[1, 3] = cross(1, 3)
    across[1, 1] = cross(1, 1)
    score(0, 2, across[0, 2])
    score(1, 0, across[1, 0])
    across[1, 2] = close(1, *far_relay_a, *far_relay_b)
    score(1, 3, across[1, 3])
    score(1, 1, across[1, 1])
    score(1, 2, across[1, 2])

    top = functools.reduce(jnp.maximum, [high for high, _, _ in stats.values()])
    factor = {i: jnp.exp(high - top) for i, (high, _, _) in stats.items()}
    inverse = 1.0 / sum(factor[i] * total for i, (_, total, _) in stats.items())
    delta = sum(factor[i] * dot for i, (_, _, dot) in stats.items()) * inverse

    crossings = {}

    def make_terms(xr):
        rotary = []
        for zr in range(NZH):
            at = pl.ds((zr * NX + xr) * chunk, chunk)
            probs = s_ref[:, at] * (factor[zr, xr] * inverse)
            probs_low = probs.astype(BF)
            grads = (probs * (gp_ref[:, at] - delta) * scale).astype(BF)
            p_ref[:, at] = probs_low
            gs_ref[:, at] = grads
            wide = lax.dot_general(
                grads, ql_ref[...], TN, preferred_element_type=F32
            ) + lax.dot_general(probs_low, gl_ref[...], TN, preferred_element_type=F32)
            rotary.append(lax.dot_general(grads, qr_ref[...], TN, preferred_element_type=F32))
            for kr in range(NC):
                part = wide[kr * NY * SR : (kr + 1) * NY * SR].astype(BF)
                for t in range(width // LANES):
                    terms[kr, xr, TILE_OF[zr][t]] = part[:, t * LANES : (t + 1) * LANES].reshape(
                        NY, SR, LANES
                    )
        for kr in range(NC):
            cut = slice(kr * NY * SR, (kr + 1) * NY * SR)
            terms[kr, xr, ROTARY_TILE] = (
                jnp.concatenate([r[cut] for r in rotary], axis=1).astype(BF).reshape(NY, SR, LANES)
            )
        crossings[xr] = send(
            terms.at[1, xr], pair_in.at[xr], p_send.at[xr], p_recv.at[xr], me.at(dk=1)
        )

    windows = (
        (pl.ds(4 * (1 - me.side), WIDE), pl.ds(0, WIDE), WIDE),
        (pl.ds(5 * me.side, NARROW), pl.ds(WIDE, NARROW), NARROW),
    )
    hops = {}

    def pair_sum(xr):
        crossings[xr].wait_recv()
        for t in range(TILES):
            x_out[xr - 1, t] = (
                terms[0, xr, t].astype(F32) + pair_in[xr, t].astype(F32)
            ).astype(BF)

    def opposite(w):
        src, dst, _ = windows[w]
        for side, dx in enumerate((1, 3)):
            hops[w, side] = send(
                x_out.at[1, src, GROUPS[side]], relay_in.at[side, dst],
                rx_send.at[w, side], rx_recv.at[w, side], me.at(dx=dx),
            )

    def direct(w):
        src, dst, _ = windows[w]
        hops[w, 2] = send(
            x_out.at[0, src, GROUPS[1]], direct_in.at[0, dst],
            rx_send.at[w, 2], rx_recv.at[w, 2], me.at(dx=1),
        )
        hops[w, 3] = send(
            x_out.at[2, src, GROUPS[0]], direct_in.at[1, dst],
            rx_send.at[w, 3], rx_recv.at[w, 3], me.at(dx=3),
        )

    def relayed(w):
        src, dst, count = windows[w]
        for side, (xi, dx) in enumerate(((0, 1), (2, 3))):
            hops[w, side].wait_recv()
            relay_out[side, dst] = (
                x_out[xi, src, GROUPS[side]].astype(F32) + relay_in[side, dst].astype(F32)
            ).astype(BF)
            hops[w, 4 + side] = send(
                relay_out.at[side, dst], sum_in.at[side, dst],
                rx_send.at[w, 4 + side], rx_recv.at[w, 4 + side], me.at(dx=dx),
            )

    make_terms(2)
    make_terms(1)
    make_terms(3)
    pair_sum(2)
    opposite(0)
    pair_sum(1)
    make_terms(0)
    pair_sum(3)
    direct(0)
    opposite(1)
    crossings[0].wait_recv()

    out = jnp.zeros((both, width), F32)
    step = 2 * chunk
    for zr in range(NZH):
        for half in range(2):
            at = pl.ds((zr * NX + 2 * half) * chunk, step)
            k_val = keys[zr, 2 * half : 2 * half + 2].reshape(step, width + rope)
            out += jnp.dot(p_ref[:, at], k_val[:, :width], preferred_element_type=F32)
    for h in range(heads):
        part = slice(h * rows, (h + 1) * rows)
        att_ref[:, h * value : (h + 1) * value] = jnp.dot(
            out[part].astype(BF), vu_ref[h], preferred_element_type=F32
        ).astype(BF)
    relayed(0)
    direct(1)
    joined = jnp.zeros((both, width), F32)
    joined_rotary = jnp.zeros((both, rope), F32)
    for zr in range(NZH):
        for half in range(2):
            at = pl.ds((zr * NX + 2 * half) * chunk, step)
            k_val = keys[zr, 2 * half : 2 * half + 2].reshape(step, width + rope)
            joined += jnp.dot(gs_ref[:, at], k_val[:, :width], preferred_element_type=F32)
            joined_rotary += jnp.dot(gs_ref[:, at], k_val[:, width:], preferred_element_type=F32)
    for h in range(heads):
        part = slice(h * rows, (h + 1) * rows)
        qg_ref[:, h * head_width : h * head_width + nope] = lax.dot_general(
            joined[part].astype(BF), ku_ref[h], NT, preferred_element_type=F32
        ).astype(BF)
        qg_ref[:, h * head_width + nope : (h + 1) * head_width] = joined_rotary[part].astype(BF)
    relayed(1)

    def summed(w, i):
        src, dst, _ = windows[w]
        tile = src.start + i
        at = dst.start + i
        base = terms[0, 0, tile].astype(F32) + pair_in[0, tile].astype(F32)
        first = base[:HALF] + sum_in[0, at].astype(F32) + direct_in[1, at].astype(F32)
        second = base[HALF:] + direct_in[0, at].astype(F32) + sum_in[1, at].astype(F32)
        return jnp.concatenate([first, second], axis=0).astype(BF)

    for i in range(2, 6):
        hops[0, i].wait_recv()
    for i in range(WIDE):
        y_far[:, i] = summed(0, i)
    ups = [
        send(
            y_far.at[slot], y_far_in.at[slot], ry_send.at[0, slot], ry_recv.at[0, slot],
            me.at(dy=SLOTS[slot], pair=1),
        )
        for slot in reversed(range(NY))
    ]
    for i in range(2, 6):
        hops[1, i].wait_recv()
    for i in range(NARROW):
        y_near[:, me.side + i] = summed(1, i)
    y_near[:, 4 * (1 - me.side)] = y_far[:, 4 * me.side]
    ups += [
        send(
            y_near.at[slot], y_near_in.at[slot - 1], ry_send.at[1, slot], ry_recv.at[1, slot],
            me.at(dy=SLOTS[slot]),
        )
        for slot in reversed(range(1, NY))
    ]
    for up in ups:
        up.wait_recv()
    part = y_near[0].astype(F32)
    for i in range(NY):
        part += y_far_in[i].astype(F32)
    for i in range(NY - 1):
        part += y_near_in[i].astype(F32)
    w_ref[...] = part

    order = me.zl // 2
    rotary = w_ref[4 * (1 - me.side)]
    z_out[0:2] = w_ref[pl.ds(2 + me.side, 2)].astype(BF)
    z_out[2] = jnp.concatenate([rotary[:, rope:], rotary[:, :rope]], axis=1).astype(BF)
    ups = [
        send(
            z_out, z_far.at[order], rz_send.at[2 + i], rz_recv.at[2 + i], me.at(far=1, mirror=True, dzl=2 * i)
        )
        for i in range(3)
    ]
    z_own[order, 0:2] = w_ref[pl.ds(me.side, 2)].astype(BF)
    z_own[order, 2] = rotary.astype(BF)
    ups += [
        send(
            z_own.at[order], z_own.at[order], rz_send.at[i], rz_recv.at[i], me.at(dzl=2 * i + 2)
        )
        for i in range(2)
    ]
    for up in ups:
        up.wait_recv()
    part = z_own[0].astype(F32)
    for i in range(1, 3):
        part += z_own[i].astype(F32)
    for i in range(3):
        part += z_far[i].astype(F32)
    final[me.side, me.k, me.x] = part.astype(BF)
    place = final.at[me.side, me.k, me.x]
    ups = [
        send(place, place, f_send.at[i], f_recv.at[i], me.at(**peer))
        for i, peer in enumerate(finals)
    ]
    for up in ups:
        up.wait_recv()
    for side in range(2):
        for t in range(2):
            at = (2 * side + t) * LANES
            grad_ref[at : at + LANES, :] = final[side, :, :, t].reshape(rows, LANES).astype(F32).T
    grad_ref[width:, :] = final[0, :, :, 2].reshape(rows, LANES).astype(F32).T[:rope]
    for copy in pending:
        copy.wait_send()


def on_device(queries, latent, block_of, key_up, value_up, out_grad):
    rows, joined = latent.shape
    heads, nope, width = key_up.shape
    value = value_up.shape[2]
    rope = joined - width
    scale = 1.0 / math.sqrt(nope + rope)
    both = heads * rows
    total = NZH * NX * NC * NY * SR
    vmem = pl.BlockSpec(memory_space=pltpu.VMEM)
    anywhere = pl.BlockSpec(memory_space=pltpu.HBM)
    dma = pltpu.SemaphoreType.DMA
    tile = (SR, LANES)
    attended, query_grad, grad = pl.pallas_call(
        functools.partial(kernel, scale, nope, rope, width, value, heads),
        out_shape=(
            pltpu.VMEM(out_grad.shape, BF),
            pltpu.VMEM(queries.shape, BF),
            pltpu.VMEM((joined, rows), F32),
        ),
        in_specs=[pl.BlockSpec(memory_space=pltpu.SMEM)] + [anywhere] * 5,
        out_specs=(vmem,) * 3,
        scratch_shapes=[
            pltpu.VMEM((2, NC, NX, 3, *tile), BF),
            pltpu.VMEM((joined, rows), BF),
            pltpu.VMEM((rows, joined), BF),
            pltpu.VMEM(queries.shape, BF),
            pltpu.VMEM(out_grad.shape, BF),
            pltpu.VMEM(key_up.shape, BF),
            pltpu.VMEM(value_up.shape, BF),
            dma((5,)),
            pltpu.VMEM((NZH, NX, NC, NY, SR, joined), BF),
            pltpu.VMEM((both, rope), BF),
            pltpu.VMEM((both, width), BF),
            pltpu.VMEM((both, width), BF),
            pltpu.VMEM((both, total), F32),
            pltpu.VMEM((both, total), F32),
            pltpu.VMEM((both, total), BF),
            pltpu.VMEM((both, total), BF),
            pltpu.VMEM((NC, NX, TILES, NY, *tile), BF),
            pltpu.VMEM((NX, TILES, NY, *tile), BF),
            pltpu.VMEM((NX - 1, TILES, NY, *tile), BF),
            pltpu.VMEM((2, TILES, HALF, *tile), BF),
            pltpu.VMEM((2, TILES, HALF, *tile), BF),
            pltpu.VMEM((2, TILES, HALF, *tile), BF),
            pltpu.VMEM((2, TILES, HALF, *tile), BF),
            pltpu.VMEM((NY, WIDE, *tile), BF),
            pltpu.VMEM((NY, WIDE, *tile), BF),
            pltpu.VMEM((NY, WIDE, *tile), BF),
            pltpu.VMEM((NY - 1, WIDE, *tile), BF),
            pltpu.VMEM((WIDE, *tile), F32),
            pltpu.VMEM((3, 3, *tile), BF),
            pltpu.VMEM((3, *tile), BF),
            pltpu.VMEM((3, 3, *tile), BF),
            dma((2, NY - 1)), dma((2, NY - 1)),
            dma, dma,
            dma((2, 8)), dma((2, 8)),
            dma((2, NX)), dma((2, NX)),
            dma((NX,)), dma((NX,)),
            dma((2, 6)), dma((2, 6)),
            dma((2, NY)), dma((2, NY)),
            dma((5,)), dma((5,)),
            dma((15,)), dma((15,)),
        ],
        compiler_params=pltpu.CompilerParams(
            collective_id=0, has_side_effects=True, vmem_limit_bytes=56 * 1024 * 1024
        ),
    )(block_of, latent.T, queries, out_grad, key_up, value_up)
    return attended, query_grad, grad.T


def solution(mesh):
    return jax.shard_map(
        on_device,
        mesh=mesh,
        in_specs=(
            P("ctx", "head"),
            P("ctx", None),
            P(),
            P("head", None, None),
            P("head", None, None),
            P("ctx", "head"),
        ),
        out_specs=(P("ctx", "head"), P("ctx", "head"), P("ctx", None)),
        check_vma=False,
    )
```

```python
import functools
import math

import jax
import jax.numpy as jnp
from jax import lax
from jax.experimental import pallas as pl
from jax.experimental.pallas import tpu as pltpu
from jax.sharding import PartitionSpec as P

MESH = pl.DeviceIdType.MESH
NX, NY, NZH, NZL, NC = 4, 8, 2, 6, 2
SR = 16
LANES = 128
SLOTS = (0, 1, 7, 2, 6, 3, 5, 4)
SLOT_OF = {j: i for i, j in enumerate(SLOTS)}
HALF = NY // 2
GROUPS = (pl.ds(0, HALF), pl.ds(HALF, HALF))
TILE_OF = ((0, 1, 5, 6), (2, 3, 7, 8))
ROTARY_TILE = 4
TILES = 9
WIDE, NARROW = 5, 4
BF = jnp.bfloat16
F32 = jnp.float32
NT = (((1,), (1,)), ((), ()))
TN = (((0,), (0,)), ((), ()))


class Place:
    def __init__(self):
        self.c = lax.axis_index("ctx")
        h = lax.axis_index("head")
        self.zh, self.y = self.c // NY, lax.rem(self.c, NY)
        self.k = lax.rem(h, NC)
        self.zl = lax.rem(h // NC, NZL)
        self.x = h // (NC * NZL)
        self.odd = lax.rem(self.zl, 2)
        self.side = lax.rem(self.zl + self.zh, 2)

    def at(self, dy=0, dx=0, dk=0, pair=0, dzl=0, far=0, mirror=False):
        zh = 1 - self.zh if far else self.zh
        y = lax.rem(self.y + dy, NY)
        x = lax.rem(self.x + dx, NX)
        k = 1 - self.k if dk else self.k
        zl = self.zl
        if mirror:
            zl = NZL - 1 - zl
        if pair:
            zl = zl + 1 - 2 * self.odd
        if dzl:
            zl = lax.rem(zl + dzl, NZL)
        return (zh * NY + y, (x * NZL + zl) * NC + k)


def kernel(
    scale, nope, rope, width, value, heads,
    blocks_hbm, lat_hbm, q_hbm, g_hbm, ku_hbm, vu_hbm,
    att_ref, qg_ref, final,
    blocks, lat_t, lat, q_ref, g_ref, ku_ref, vu_ref, in_sem,
    keys, qr_ref, ql_ref, gl_ref, s_ref, gp_ref, p_ref, gs_ref,
    terms, pair_in, x_out, relay_in, direct_in, relay_out, sum_in,
    y_far, y_near, y_far_in, y_near_in, w_ref, z_own, z_out, z_far,
    y_send, y_recv, m_send, m_recv, x_send, x_recv, d_send, d_recv,
    p_send, p_recv, rx_send, rx_recv, ry_send, ry_recv, rz_send, rz_recv, f_send, f_recv,
):
    me = Place()
    rows = q_ref.shape[0]
    both = heads * rows
    head_width = nope + rope
    chunk = NC * NY * SR
    pending = []

    def send(src, dst, send_sem, recv_sem, peer):
        copy = pltpu.make_async_remote_copy(
            src_ref=src, dst_ref=dst, send_sem=send_sem, recv_sem=recv_sem,
            device_id=peer, device_id_type=MESH,
        )
        copy.start()
        pending.append(copy)
        return copy

    finals = [
        dict(pair=pair, dk=dk, dx=dx)
        for pair in range(2) for dk in range(NC) for dx in range(NX) if pair or dk or dx
    ]
    peers = (
        [dict(dy=d) for d in range(1, NY)]
        + [dict(dy=d, pair=1) for d in range(1, NY)]
        + finals
        + [dict(dzl=2), dict(dzl=4)]
        + [dict(far=1, mirror=True, dzl=d) for d in (0, 2, 4)]
    )
    barrier = pltpu.get_barrier_semaphore()
    for peer in peers:
        pl.semaphore_signal(barrier, inc=1, device_id=me.at(**peer), device_id_type=MESH)

    loads = [
        pltpu.make_async_copy(src, dst, in_sem.at[i])
        for i, (src, dst) in enumerate(
            (
                (lat_hbm, lat_t), (q_hbm, q_ref), (ku_hbm, ku_ref), (g_hbm, g_ref),
                (vu_hbm, vu_ref), (blocks_hbm, blocks),
            )
        )
    ]
    for load in loads:
        load.start()
    loads[0].wait()
    for t in range(0, width, LANES):
        lat[:, t : t + LANES] = lat_t[t : t + LANES, :].T
    lat[:, width:] = lat_t[width:, :].T
    mine = pl.ds(pl.multiple_of((me.k * NX + me.x) * SR, SR), SR)
    keys[0, 0, 0, 0] = lat[mine, :]

    pl.semaphore_wait(barrier, len(peers))

    own = lat.at[mine, :]
    to_mirror = send(own, keys.at[1, 0, 0, 0], m_send, m_recv, me.at(far=1, mirror=True))

    def along_y(zr, src):
        return {
            NY - d: send(
                src, keys.at[zr, 0, 0, SLOT_OF[NY - d]],
                y_send.at[zr, d - 1], y_recv.at[zr, d - 1], me.at(dy=d),
            )
            for d in (7, 1, 6, 2, 5, 3, 4)
        }

    def x_copy(zr, i, src_x, dst_x, part, dx):
        return send(
            keys.at[zr, src_x, 0, part], keys.at[zr, dst_x, 0, part],
            x_send.at[zr, i], x_recv.at[zr, i], me.at(dx=dx),
        )

    def cross(zr, xr):
        return send(
            keys.at[zr, xr, 0], keys.at[zr, xr, 1], d_send.at[zr, xr], d_recv.at[zr, xr],
            me.at(dk=1),
        )

    def spread(zr, group, arrivals):
        for j in SLOTS[group * HALF : (group + 1) * HALF]:
            if j:
                arrivals[j].wait_recv()
        part = GROUPS[group]
        return (
            x_copy(zr, 4 * group, 0, 3, part, 1),
            x_copy(zr, 4 * group + 1, 0, 1, part, 3),
        )

    def relay(zr, group, moves):
        start = group * HALF
        moves[0].wait_recv()
        right = x_copy(zr, 4 * group + 2, 3, 2, pl.ds(start, HALF // 2), 1)
        moves[1].wait_recv()
        left = x_copy(zr, 4 * group + 3, 1, 2, pl.ds(start + HALF // 2, HALF // 2), 3)
        return right, left

    def close(zr, *relays):
        for copy in relays:
            copy.wait_recv()
        return cross(zr, 2)

    stats = {}

    def score(zr, xr, arrived):
        arrived.wait_recv()
        at = pl.ds((zr * NX + xr) * chunk, chunk)
        k_val = keys[zr, xr].reshape(chunk, width + rope)
        part = lax.dot_general(
            ql_ref[...], k_val[:, :width], NT, preferred_element_type=F32
        ) + lax.dot_general(qr_ref[...], k_val[:, width:], NT, preferred_element_type=F32)
        key_pos = starts[zr] + lax.rem(me.x + xr, NX) * SR
        seen = key_pos <= my_pos
        part = part * scale
        part = jnp.concatenate(
            [jnp.where(seen, part[h * rows : (h + 1) * rows], -1e30) for h in range(heads)], axis=0
        )
        high = jnp.max(part, axis=1, keepdims=True)
        expo = jnp.exp(part - high)
        back = lax.dot_general(gl_ref[...], k_val[:, :width], NT, preferred_element_type=F32)
        s_ref[:, at] = expo
        gp_ref[:, at] = back
        stats[zr, xr] = (
            high,
            jnp.sum(expo, axis=1, keepdims=True),
            jnp.sum(expo * back, axis=1, keepdims=True),
        )

    near = along_y(0, own)

    for load in loads[1:]:
        load.wait()
    for h in range(heads):
        at = pl.ds(h * rows, rows)
        qn = q_ref[:, h * head_width : h * head_width + nope]
        ql_ref[at, :] = jnp.dot(qn, ku_ref[h], preferred_element_type=F32).astype(BF)
        qr_ref[at, :] = q_ref[:, h * head_width + nope : (h + 1) * head_width]
        gl_ref[at, :] = lax.dot_general(
            g_ref[:, h * value : (h + 1) * value], vu_ref[h], NT, preferred_element_type=F32
        ).astype(BF)
    block = rows // 2
    row = lax.broadcasted_iota(jnp.int32, (rows, 1), 0)
    my_pos = jnp.where(row < block, blocks[2 * me.c], blocks[2 * me.c + 1]) * block + lax.rem(
        row, block
    )
    lane = lax.broadcasted_iota(jnp.int32, (1, chunk), 1)
    starts = []
    for zr in range(NZH):
        start = jnp.zeros((1, chunk), jnp.int32)
        for kr in range(NC):
            for slot, j in enumerate(SLOTS):
                zh = 1 - me.zh if zr else me.zh
                k = 1 - me.k if kr else me.k
                owner = zh * NY + lax.rem(me.y + j, NY)
                start = jnp.where(
                    lane // SR == kr * NY + slot, blocks[2 * owner + k] * block, start
                )
        starts.append(start + lax.rem(lane, SR))

    near_a = spread(0, 0, near)
    to_mirror.wait_recv()
    far = along_y(1, keys.at[1, 0, 0, 0])
    near_b = spread(0, 1, near)
    across = {(0, 0): cross(0, 0)}
    near_relay_a = relay(0, 0, near_a)
    far_a = spread(1, 0, far)
    near_relay_b = relay(0, 1, near_b)
    across[0, 3] = cross(0, 3)
    across[0, 1] = cross(0, 1)
    score(0, 0, across[0, 0])
    far_b = spread(1, 1, far)
    across[1, 0] = cross(1, 0)
    across[0, 2] = close(0, *near_relay_a, *near_relay_b)
    far_relay_a = relay(1, 0, far_a)
    score(0, 3, across[0, 3])
    score(0, 1, across[0, 1])
    far_relay_b = relay(1, 1, far_b)
    across[1, 3] = cross(1, 3)
    across[1, 1] = cross(1, 1)
    score(0, 2, across[0, 2])
    score(1, 0, across[1, 0])
    across[1, 2] = close(1, *far_relay_a, *far_relay_b)
    score(1, 3, across[1, 3])
    score(1, 1, across[1, 1])
    score(1, 2, across[1, 2])

    top = functools.reduce(jnp.maximum, [high for high, _, _ in stats.values()])
    factor = {i: jnp.exp(high - top) for i, (high, _, _) in stats.items()}
    inverse = 1.0 / sum(factor[i] * total for i, (_, total, _) in stats.items())
    delta = sum(factor[i] * dot for i, (_, _, dot) in stats.items()) * inverse

    crossings = {}

    def make_terms(xr):
        rotary = []
        for zr in range(NZH):
            at = pl.ds((zr * NX + xr) * chunk, chunk)
            probs = s_ref[:, at] * (factor[zr, xr] * inverse)
            probs_low = probs.astype(BF)
            grads = (probs * (gp_ref[:, at] - delta) * scale).astype(BF)
            p_ref[:, at] = probs_low
            gs_ref[:, at] = grads
            wide = lax.dot_general(
                grads, ql_ref[...], TN, preferred_element_type=F32
            ) + lax.dot_general(probs_low, gl_ref[...], TN, preferred_element_type=F32)
            rotary.append(lax.dot_general(grads, qr_ref[...], TN, preferred_element_type=F32))
            for kr in range(NC):
                part = wide[kr * NY * SR : (kr + 1) * NY * SR].astype(BF)
                for t in range(width // LANES):
                    terms[kr, xr, TILE_OF[zr][t]] = part[:, t * LANES : (t + 1) * LANES].reshape(
                        NY, SR, LANES
                    )
        for kr in range(NC):
            cut = slice(kr * NY * SR, (kr + 1) * NY * SR)
            terms[kr, xr, ROTARY_TILE] = (
                jnp.concatenate([r[cut] for r in rotary], axis=1).astype(BF).reshape(NY, SR, LANES)
            )
        crossings[xr] = send(
            terms.at[1, xr], pair_in.at[xr], p_send.at[xr], p_recv.at[xr], me.at(dk=1)
        )

    windows = (
        (pl.ds(4 * (1 - me.side), WIDE), pl.ds(0, WIDE), WIDE),
        (pl.ds(5 * me.side, NARROW), pl.ds(WIDE, NARROW), NARROW),
    )
    hops = {}

    def pair_sum(xr):
        crossings[xr].wait_recv()
        for t in range(TILES):
            x_out[xr - 1, t] = (
                terms[0, xr, t].astype(F32) + pair_in[xr, t].astype(F32)
            ).astype(BF)

    def opposite(w):
        src, dst, _ = windows[w]
        for side, dx in enumerate((1, 3)):
            hops[w, side] = send(
                x_out.at[1, src, GROUPS[side]], relay_in.at[side, dst],
                rx_send.at[w, side], rx_recv.at[w, side], me.at(dx=dx),
            )

    def direct(w):
        src, dst, _ = windows[w]
        hops[w, 2] = send(
            x_out.at[0, src, GROUPS[1]], direct_in.at[0, dst],
            rx_send.at[w, 2], rx_recv.at[w, 2], me.at(dx=1),
        )
        hops[w, 3] = send(
            x_out.at[2, src, GROUPS[0]], direct_in.at[1, dst],
            rx_send.at[w, 3], rx_recv.at[w, 3], me.at(dx=3),
        )

    def relayed(w):
        src, dst, count = windows[w]
        for side, (xi, dx) in enumerate(((0, 1), (2, 3))):
            hops[w, side].wait_recv()
            relay_out[side, dst] = (
                x_out[xi, src, GROUPS[side]].astype(F32) + relay_in[side, dst].astype(F32)
            ).astype(BF)
            hops[w, 4 + side] = send(
                relay_out.at[side, dst], sum_in.at[side, dst],
                rx_send.at[w, 4 + side], rx_recv.at[w, 4 + side], me.at(dx=dx),
            )

    make_terms(2)
    make_terms(1)
    make_terms(3)
    pair_sum(2)
    opposite(0)
    pair_sum(1)
    make_terms(0)
    pair_sum(3)
    direct(0)
    opposite(1)
    crossings[0].wait_recv()

    out = jnp.zeros((both, width), F32)
    step = 2 * chunk
    for zr in range(NZH):
        for half in range(2):
            at = pl.ds((zr * NX + 2 * half) * chunk, step)
            k_val = keys[zr, 2 * half : 2 * half + 2].reshape(step, width + rope)
            out += jnp.dot(p_ref[:, at], k_val[:, :width], preferred_element_type=F32)
    for h in range(heads):
        part = slice(h * rows, (h + 1) * rows)
        att_ref[:, h * value : (h + 1) * value] = jnp.dot(
            out[part].astype(BF), vu_ref[h], preferred_element_type=F32
        ).astype(BF)
    relayed(0)
    direct(1)
    joined = jnp.zeros((both, width), F32)
    joined_rotary = jnp.zeros((both, rope), F32)
    for zr in range(NZH):
        for half in range(2):
            at = pl.ds((zr * NX + 2 * half) * chunk, step)
            k_val = keys[zr, 2 * half : 2 * half + 2].reshape(step, width + rope)
            joined += jnp.dot(gs_ref[:, at], k_val[:, :width], preferred_element_type=F32)
            joined_rotary += jnp.dot(gs_ref[:, at], k_val[:, width:], preferred_element_type=F32)
    for h in range(heads):
        part = slice(h * rows, (h + 1) * rows)
        qg_ref[:, h * head_width : h * head_width + nope] = lax.dot_general(
            joined[part].astype(BF), ku_ref[h], NT, preferred_element_type=F32
        ).astype(BF)
        qg_ref[:, h * head_width + nope : (h + 1) * head_width] = joined_rotary[part].astype(BF)
    relayed(1)

    def summed(w, i):
        src, dst, _ = windows[w]
        tile = src.start + i
        at = dst.start + i
        base = terms[0, 0, tile].astype(F32) + pair_in[0, tile].astype(F32)
        first = base[:HALF] + sum_in[0, at].astype(F32) + direct_in[1, at].astype(F32)
        second = base[HALF:] + direct_in[0, at].astype(F32) + sum_in[1, at].astype(F32)
        return jnp.concatenate([first, second], axis=0).astype(BF)

    for i in range(2, 6):
        hops[0, i].wait_recv()
    for i in range(WIDE):
        y_far[:, i] = summed(0, i)
    ups = [
        send(
            y_far.at[slot], y_far_in.at[slot], ry_send.at[0, slot], ry_recv.at[0, slot],
            me.at(dy=SLOTS[slot], pair=1),
        )
        for slot in reversed(range(NY))
    ]
    for i in range(2, 6):
        hops[1, i].wait_recv()
    for i in range(NARROW):
        y_near[:, me.side + i] = summed(1, i)
    y_near[:, 4 * (1 - me.side)] = y_far[:, 4 * me.side]
    ups += [
        send(
            y_near.at[slot], y_near_in.at[slot - 1], ry_send.at[1, slot], ry_recv.at[1, slot],
            me.at(dy=SLOTS[slot]),
        )
        for slot in reversed(range(1, NY))
    ]
    for up in ups:
        up.wait_recv()
    part = y_near[0].astype(F32)
    for i in range(NY):
        part += y_far_in[i].astype(F32)
    for i in range(NY - 1):
        part += y_near_in[i].astype(F32)
    w_ref[...] = part

    order = me.zl // 2
    rotary = w_ref[4 * (1 - me.side)]
    z_out[0:2] = w_ref[pl.ds(2 + me.side, 2)].astype(BF)
    z_out[2] = jnp.concatenate([rotary[:, rope:], rotary[:, :rope]], axis=1).astype(BF)
    ups = [
        send(
            z_out, z_far.at[order], rz_send.at[2 + i], rz_recv.at[2 + i], me.at(far=1, mirror=True, dzl=2 * i)
        )
        for i in range(3)
    ]
    z_own[order, 0:2] = w_ref[pl.ds(me.side, 2)].astype(BF)
    z_own[order, 2] = rotary.astype(BF)
    ups += [
        send(
            z_own.at[order], z_own.at[order], rz_send.at[i], rz_recv.at[i], me.at(dzl=2 * i + 2)
        )
        for i in range(2)
    ]
    for up in ups:
        up.wait_recv()
    part = z_own[0].astype(F32)
    for i in range(1, 3):
        part += z_own[i].astype(F32)
    for i in range(3):
        part += z_far[i].astype(F32)
    final[me.side, me.k, me.x] = part.astype(BF)
    place = final.at[me.side, me.k, me.x]
    ups = [
        send(place, place, f_send.at[i], f_recv.at[i], me.at(**peer))
        for i, peer in enumerate(finals)
    ]
    for copy in pending[: -len(finals)]:
        copy.wait_send()
    for up in ups:
        up.wait()


def write_kernel(rope, att, qg, final, att_hbm, qg_hbm, grad_hbm, grad, sem):
    copies = [
        pltpu.make_async_copy(src, dst, sem.at[i])
        for i, (src, dst) in enumerate(((att, att_hbm), (qg, qg_hbm), (grad, grad_hbm)))
    ]
    copies[0].start()
    copies[1].start()
    width, rows = grad.shape
    for side in range(2):
        for t in range(2):
            at = (2 * side + t) * LANES
            grad[at : at + LANES, :] = final[side, :, :, t].reshape(rows, LANES).astype(F32).T
    grad[width - rope :, :] = final[0, :, :, 2].reshape(rows, LANES).astype(F32).T[:rope]
    copies[2].start()
    for copy in copies:
        copy.wait()


def on_device(queries, latent, block_of, key_up, value_up, out_grad):
    rows, joined = latent.shape
    heads, nope, width = key_up.shape
    value = value_up.shape[2]
    rope = joined - width
    scale = 1.0 / math.sqrt(nope + rope)
    both = heads * rows
    total = NZH * NX * NC * NY * SR
    vmem = pl.BlockSpec(memory_space=pltpu.VMEM)
    anywhere = pl.BlockSpec(memory_space=pl.ANY)
    dma = pltpu.SemaphoreType.DMA
    tile = (SR, LANES)
    results = pl.pallas_call(
        functools.partial(kernel, scale, nope, rope, width, value, heads),
        out_shape=(
            pltpu.VMEM(out_grad.shape, BF),
            pltpu.VMEM(queries.shape, BF),
            pltpu.VMEM((2, NC, NX, 3, *tile), BF),
        ),
        in_specs=[anywhere] * 6,
        out_specs=(vmem,) * 3,
        scratch_shapes=[
            pltpu.SMEM(block_of.shape, jnp.int32),
            pltpu.VMEM((joined, rows), BF),
            pltpu.VMEM((rows, joined), BF),
            pltpu.VMEM(queries.shape, BF),
            pltpu.VMEM(out_grad.shape, BF),
            pltpu.VMEM(key_up.shape, BF),
            pltpu.VMEM(value_up.shape, BF),
            dma((6,)),
            pltpu.VMEM((NZH, NX, NC, NY, SR, joined), BF),
            pltpu.VMEM((both, rope), BF),
            pltpu.VMEM((both, width), BF),
            pltpu.VMEM((both, width), BF),
            pltpu.VMEM((both, total), F32),
            pltpu.VMEM((both, total), F32),
            pltpu.VMEM((both, total), BF),
            pltpu.VMEM((both, total), BF),
            pltpu.VMEM((NC, NX, TILES, NY, *tile), BF),
            pltpu.VMEM((NX, TILES, NY, *tile), BF),
            pltpu.VMEM((NX - 1, TILES, NY, *tile), BF),
            pltpu.VMEM((2, TILES, HALF, *tile), BF),
            pltpu.VMEM((2, TILES, HALF, *tile), BF),
            pltpu.VMEM((2, TILES, HALF, *tile), BF),
            pltpu.VMEM((2, TILES, HALF, *tile), BF),
            pltpu.VMEM((NY, WIDE, *tile), BF),
            pltpu.VMEM((NY, WIDE, *tile), BF),
            pltpu.VMEM((NY, WIDE, *tile), BF),
            pltpu.VMEM((NY - 1, WIDE, *tile), BF),
            pltpu.VMEM((WIDE, *tile), F32),
            pltpu.VMEM((3, 3, *tile), BF),
            pltpu.VMEM((3, *tile), BF),
            pltpu.VMEM((3, 3, *tile), BF),
            dma((2, NY - 1)), dma((2, NY - 1)),
            dma, dma,
            dma((2, 8)), dma((2, 8)),
            dma((2, NX)), dma((2, NX)),
            dma((NX,)), dma((NX,)),
            dma((2, 6)), dma((2, 6)),
            dma((2, NY)), dma((2, NY)),
            dma((5,)), dma((5,)),
            dma((15,)), dma((15,)),
        ],
        compiler_params=pltpu.CompilerParams(
            collective_id=0, has_side_effects=True, vmem_limit_bytes=56 * 1024 * 1024
        ),
    )(block_of, latent.T, queries, out_grad, key_up, value_up)

    attended, query_grad, grad = pl.pallas_call(
        functools.partial(write_kernel, rope),
        out_shape=(
            jax.ShapeDtypeStruct(out_grad.shape, BF),
            jax.ShapeDtypeStruct(queries.shape, BF),
            jax.ShapeDtypeStruct((joined, rows), F32),
        ),
        in_specs=[vmem] * 3,
        out_specs=(anywhere,) * 3,
        scratch_shapes=[pltpu.VMEM((joined, rows), F32), dma((3,))],
    )(*(pltpu.with_memory_space_constraint(a, pltpu.VMEM) for a in results))
    return attended, query_grad, grad.T


def solution(mesh):
    return jax.shard_map(
        on_device,
        mesh=mesh,
        in_specs=(
            P("ctx", "head"),
            P("ctx", None),
            P(),
            P("head", None, None),
            P("head", None, None),
            P("ctx", "head"),
        ),
        out_specs=(P("ctx", "head"), P("ctx", "head"), P("ctx", None)),
        check_vma=False,
    )
```

```python
import functools
import math

import jax
import jax.numpy as jnp
from jax import lax
from jax.experimental import pallas as pl
from jax.experimental.pallas import tpu as pltpu
from jax.sharding import PartitionSpec as P

MESH = pl.DeviceIdType.MESH
NX, NY, NZH, NZL, NC = 4, 8, 2, 6, 2
SR = 16
LANES = 128
SLOTS = (0, 1, 7, 2, 6, 3, 5, 4)
SLOT_OF = {j: i for i, j in enumerate(SLOTS)}
HALF = NY // 2
SPANS = ((0, 2, 3), (3, 4, 5), (5, 6, 8))
GROUPS = (pl.ds(0, HALF), pl.ds(HALF, HALF))
TILE_OF = ((0, 1, 5, 6), (2, 3, 7, 8))
ROTARY_TILE = 4
TILES = 9
WIDE, NARROW = 5, 4
BF = jnp.bfloat16
F32 = jnp.float32
NT = (((1,), (1,)), ((), ()))
TN = (((0,), (0,)), ((), ()))


class Place:
    def __init__(self):
        self.c = lax.axis_index("ctx")
        h = lax.axis_index("head")
        self.zh, self.y = self.c // NY, lax.rem(self.c, NY)
        self.k = lax.rem(h, NC)
        self.zl = lax.rem(h // NC, NZL)
        self.x = h // (NC * NZL)
        self.odd = lax.rem(self.zl, 2)
        self.side = lax.rem(self.zl + self.zh, 2)

    def at(self, dy=0, dx=0, dk=0, pair=0, dzl=0, far=0, mirror=False):
        zh = 1 - self.zh if far else self.zh
        y = lax.rem(self.y + dy, NY)
        x = lax.rem(self.x + dx, NX)
        k = 1 - self.k if dk else self.k
        zl = self.zl
        if mirror:
            zl = NZL - 1 - zl
        if pair:
            zl = zl + 1 - 2 * self.odd
        if dzl:
            zl = lax.rem(zl + dzl, NZL)
        return (zh * NY + y, (x * NZL + zl) * NC + k)


def kernel(
    scale, nope, rope, width, value, heads,
    blocks_hbm, lat_hbm, q_hbm, g_hbm, ku_hbm, vu_hbm,
    att_ref, qg_ref, final,
    blocks, lat_t, lat, q_ref, g_ref, ku_ref, vu_ref, in_sem,
    keys, qr_ref, ql_ref, gl_ref, s_ref, gp_ref, p_ref, gs_ref,
    terms, pair_in, x_out, relay_in, direct_in, relay_out, sum_in,
    y_far, y_near, y_far_in, y_near_in, w_ref, z_own, z_out, z_far,
    y_send, y_recv, m_send, m_recv, x_send, x_recv, d_send, d_recv,
    p_send, p_recv, rx_send, rx_recv, ry_send, ry_recv, rz_send, rz_recv, f_send, f_recv,
):
    me = Place()
    rows = q_ref.shape[0]
    both = heads * rows
    head_width = nope + rope
    chunk = NC * NY * SR
    pending = []

    def send(src, dst, send_sem, recv_sem, peer):
        copy = pltpu.make_async_remote_copy(
            src_ref=src, dst_ref=dst, send_sem=send_sem, recv_sem=recv_sem,
            device_id=peer, device_id_type=MESH,
        )
        copy.start()
        pending.append(copy)
        return copy

    finals = [
        dict(pair=pair, dk=dk, dx=dx)
        for pair in range(2) for dk in range(NC) for dx in range(NX) if pair or dk or dx
    ]
    finals.sort(key=lambda p: -(p["pair"] + min(p["dx"], NX - p["dx"])))
    peers = (
        [dict(dy=d) for d in range(1, NY)]
        + [dict(dy=d, pair=1) for d in range(1, NY)]
        + finals
        + [dict(dzl=2), dict(dzl=4)]
        + [dict(far=1, mirror=True, dzl=d) for d in (0, 2, 4)]
    )
    barrier = pltpu.get_barrier_semaphore()
    for peer in peers:
        pl.semaphore_signal(barrier, inc=1, device_id=me.at(**peer), device_id_type=MESH)

    loads = [
        pltpu.make_async_copy(src, dst, in_sem.at[i])
        for i, (src, dst) in enumerate(
            (
                (lat_hbm, lat_t), (q_hbm, q_ref), (ku_hbm, ku_ref), (g_hbm, g_ref),
                (vu_hbm, vu_ref), (blocks_hbm, blocks),
            )
        )
    ]
    for load in loads:
        load.start()
    loads[0].wait()
    for t in range(0, width, LANES):
        lat[:, t : t + LANES] = lat_t[t : t + LANES, :].T
    lat[:, width:] = lat_t[width:, :].T
    mine = pl.ds(pl.multiple_of((me.k * NX + me.x) * SR, SR), SR)
    keys[0, 0, 0, 0] = lat[mine, :]

    pl.semaphore_wait(barrier, len(peers))

    own = lat.at[mine, :]
    to_mirror = send(own, keys.at[1, 0, 0, 0], m_send, m_recv, me.at(far=1, mirror=True))

    def along_y(zr, src):
        return {
            NY - d: send(
                src, keys.at[zr, 0, 0, SLOT_OF[NY - d]],
                y_send.at[zr, d - 1], y_recv.at[zr, d - 1], me.at(dy=d),
            )
            for d in (7, 1, 6, 2, 5, 3, 4)
        }

    def x_copy(zr, i, src_x, dst_x, part, dx):
        return send(
            keys.at[zr, src_x, 0, part], keys.at[zr, dst_x, 0, part],
            x_send.at[zr, i], x_recv.at[zr, i], me.at(dx=dx),
        )

    def cross(zr, xr):
        return send(
            keys.at[zr, xr, 0], keys.at[zr, xr, 1], d_send.at[zr, xr], d_recv.at[zr, xr],
            me.at(dk=1),
        )

    def spread(zr, group, arrivals):
        start, _, stop = SPANS[group]
        for j in SLOTS[start:stop]:
            if j:
                arrivals[j].wait_recv()
        part = pl.ds(start, stop - start)
        return (
            x_copy(zr, 4 * group, 0, 3, part, 1),
            x_copy(zr, 4 * group + 1, 0, 1, part, 3),
        )

    def relay(zr, group, moves):
        start, middle, stop = SPANS[group]
        moves[0].wait_recv()
        right = x_copy(zr, 4 * group + 2, 3, 2, pl.ds(start, middle - start), 1)
        moves[1].wait_recv()
        left = x_copy(zr, 4 * group + 3, 1, 2, pl.ds(middle, stop - middle), 3)
        return right, left

    def close(zr, *relays):
        for copy in relays:
            copy.wait_recv()
        return cross(zr, 2)

    stats = {}

    def score(zr, xr, arrived):
        arrived.wait_recv()
        at = pl.ds((zr * NX + xr) * chunk, chunk)
        k_val = keys[zr, xr].reshape(chunk, width + rope)
        part = lax.dot_general(
            ql_ref[...], k_val[:, :width], NT, preferred_element_type=F32
        ) + lax.dot_general(qr_ref[...], k_val[:, width:], NT, preferred_element_type=F32)
        key_pos = starts[zr] + lax.rem(me.x + xr, NX) * SR
        seen = key_pos <= my_pos
        part = part * scale
        part = jnp.concatenate(
            [jnp.where(seen, part[h * rows : (h + 1) * rows], -1e30) for h in range(heads)], axis=0
        )
        high = jnp.max(part, axis=1, keepdims=True)
        expo = jnp.exp(part - high)
        back = lax.dot_general(gl_ref[...], k_val[:, :width], NT, preferred_element_type=F32)
        s_ref[:, at] = expo
        gp_ref[:, at] = back
        stats[zr, xr] = (
            high,
            jnp.sum(expo, axis=1, keepdims=True),
            jnp.sum(expo * back, axis=1, keepdims=True),
        )

    near = along_y(0, own)

    for load in loads[1:]:
        load.wait()
    for h in range(heads):
        at = pl.ds(h * rows, rows)
        qn = q_ref[:, h * head_width : h * head_width + nope]
        ql_ref[at, :] = jnp.dot(qn, ku_ref[h], preferred_element_type=F32).astype(BF)
        qr_ref[at, :] = q_ref[:, h * head_width + nope : (h + 1) * head_width]
        gl_ref[at, :] = lax.dot_general(
            g_ref[:, h * value : (h + 1) * value], vu_ref[h], NT, preferred_element_type=F32
        ).astype(BF)
    block = rows // 2
    row = lax.broadcasted_iota(jnp.int32, (rows, 1), 0)
    my_pos = jnp.where(row < block, blocks[2 * me.c], blocks[2 * me.c + 1]) * block + lax.rem(
        row, block
    )
    lane = lax.broadcasted_iota(jnp.int32, (1, chunk), 1)
    starts = []
    for zr in range(NZH):
        start = jnp.zeros((1, chunk), jnp.int32)
        for kr in range(NC):
            for slot, j in enumerate(SLOTS):
                zh = 1 - me.zh if zr else me.zh
                k = 1 - me.k if kr else me.k
                owner = zh * NY + lax.rem(me.y + j, NY)
                start = jnp.where(
                    lane // SR == kr * NY + slot, blocks[2 * owner + k] * block, start
                )
        starts.append(start + lax.rem(lane, SR))

    near_moves = [spread(0, 0, near), spread(0, 1, near)]
    to_mirror.wait_recv()
    far = along_y(1, keys.at[1, 0, 0, 0])
    near_moves.append(spread(0, 2, near))
    across = {(0, 0): cross(0, 0)}
    near_relays = relay(0, 0, near_moves[0]) + relay(0, 1, near_moves[1])
    far_moves = [spread(1, 0, far)]
    near_relays += relay(0, 2, near_moves[2])
    across[0, 3] = cross(0, 3)
    across[0, 1] = cross(0, 1)
    score(0, 0, across[0, 0])
    far_moves += [spread(1, 1, far), spread(1, 2, far)]
    across[1, 0] = cross(1, 0)
    far_relays = relay(1, 0, far_moves[0])
    across[0, 2] = close(0, *near_relays)
    score(0, 3, across[0, 3])
    far_relays += relay(1, 1, far_moves[1])
    score(0, 1, across[0, 1])
    far_relays += relay(1, 2, far_moves[2])
    across[1, 3] = cross(1, 3)
    across[1, 1] = cross(1, 1)
    score(0, 2, across[0, 2])
    score(1, 0, across[1, 0])
    across[1, 2] = close(1, *far_relays)
    score(1, 3, across[1, 3])
    score(1, 1, across[1, 1])
    score(1, 2, across[1, 2])

    top = functools.reduce(jnp.maximum, [high for high, _, _ in stats.values()])
    factor = {i: jnp.exp(high - top) for i, (high, _, _) in stats.items()}
    inverse = 1.0 / sum(factor[i] * total for i, (_, total, _) in stats.items())
    delta = sum(factor[i] * dot for i, (_, _, dot) in stats.items()) * inverse

    crossings = {}

    def make_terms(xr):
        rotary = []
        for zr in range(NZH):
            at = pl.ds((zr * NX + xr) * chunk, chunk)
            probs = s_ref[:, at] * (factor[zr, xr] * inverse)
            probs_low = probs.astype(BF)
            grads = (probs * (gp_ref[:, at] - delta) * scale).astype(BF)
            p_ref[:, at] = probs_low
            gs_ref[:, at] = grads
            wide = lax.dot_general(
                grads, ql_ref[...], TN, preferred_element_type=F32
            ) + lax.dot_general(probs_low, gl_ref[...], TN, preferred_element_type=F32)
            rotary.append(lax.dot_general(grads, qr_ref[...], TN, preferred_element_type=F32))
            for kr in range(NC):
                part = wide[kr * NY * SR : (kr + 1) * NY * SR].astype(BF)
                for t in range(width // LANES):
                    terms[kr, xr, TILE_OF[zr][t]] = part[:, t * LANES : (t + 1) * LANES].reshape(
                        NY, SR, LANES
                    )
        for kr in range(NC):
            cut = slice(kr * NY * SR, (kr + 1) * NY * SR)
            terms[kr, xr, ROTARY_TILE] = (
                jnp.concatenate([r[cut] for r in rotary], axis=1).astype(BF).reshape(NY, SR, LANES)
            )
        crossings[xr] = send(
            terms.at[1, xr], pair_in.at[xr], p_send.at[xr], p_recv.at[xr], me.at(dk=1)
        )

    windows = (
        (pl.ds(4 * (1 - me.side), WIDE), pl.ds(0, WIDE), WIDE),
        (pl.ds(5 * me.side, NARROW), pl.ds(WIDE, NARROW), NARROW),
    )
    hops = {}

    def pair_sum(xr):
        crossings[xr].wait_recv()
        for t in range(TILES):
            x_out[xr - 1, t] = (
                terms[0, xr, t].astype(F32) + pair_in[xr, t].astype(F32)
            ).astype(BF)

    def opposite(w):
        src, dst, _ = windows[w]
        for side, dx in enumerate((1, 3)):
            hops[w, side] = send(
                x_out.at[1, src, GROUPS[side]], relay_in.at[side, dst],
                rx_send.at[w, side], rx_recv.at[w, side], me.at(dx=dx),
            )

    def direct(w):
        src, dst, _ = windows[w]
        hops[w, 2] = send(
            x_out.at[0, src, GROUPS[1]], direct_in.at[0, dst],
            rx_send.at[w, 2], rx_recv.at[w, 2], me.at(dx=1),
        )
        hops[w, 3] = send(
            x_out.at[2, src, GROUPS[0]], direct_in.at[1, dst],
            rx_send.at[w, 3], rx_recv.at[w, 3], me.at(dx=3),
        )

    def relayed(w):
        src, dst, count = windows[w]
        for side, (xi, dx) in enumerate(((0, 1), (2, 3))):
            hops[w, side].wait_recv()
            relay_out[side, dst] = (
                x_out[xi, src, GROUPS[side]].astype(F32) + relay_in[side, dst].astype(F32)
            ).astype(BF)
            hops[w, 4 + side] = send(
                relay_out.at[side, dst], sum_in.at[side, dst],
                rx_send.at[w, 4 + side], rx_recv.at[w, 4 + side], me.at(dx=dx),
            )

    make_terms(2)
    make_terms(1)
    make_terms(3)
    pair_sum(2)
    opposite(0)
    pair_sum(1)
    make_terms(0)
    pair_sum(3)
    direct(0)
    opposite(1)

    out = jnp.zeros((both, width), F32)
    step = 2 * chunk
    for zr in range(NZH):
        for half in range(2):
            at = pl.ds((zr * NX + 2 * half) * chunk, step)
            k_val = keys[zr, 2 * half : 2 * half + 2].reshape(step, width + rope)
            out += jnp.dot(p_ref[:, at], k_val[:, :width], preferred_element_type=F32)
    for h in range(heads):
        part = slice(h * rows, (h + 1) * rows)
        att_ref[:, h * value : (h + 1) * value] = jnp.dot(
            out[part].astype(BF), vu_ref[h], preferred_element_type=F32
        ).astype(BF)
    relayed(0)
    direct(1)
    joined = jnp.zeros((both, width), F32)
    joined_rotary = jnp.zeros((both, rope), F32)
    for zr in range(NZH):
        for half in range(2):
            at = pl.ds((zr * NX + 2 * half) * chunk, step)
            k_val = keys[zr, 2 * half : 2 * half + 2].reshape(step, width + rope)
            joined += jnp.dot(gs_ref[:, at], k_val[:, :width], preferred_element_type=F32)
            joined_rotary += jnp.dot(gs_ref[:, at], k_val[:, width:], preferred_element_type=F32)
    for h in range(heads):
        part = slice(h * rows, (h + 1) * rows)
        qg_ref[:, h * head_width : h * head_width + nope] = lax.dot_general(
            joined[part].astype(BF), ku_ref[h], NT, preferred_element_type=F32
        ).astype(BF)
        qg_ref[:, h * head_width + nope : (h + 1) * head_width] = joined_rotary[part].astype(BF)
    relayed(1)

    def summed(w, i):
        src, dst, _ = windows[w]
        tile = src.start + i
        at = dst.start + i
        base = terms[0, 0, tile].astype(F32) + pair_in[0, tile].astype(F32)
        first = base[:HALF] + sum_in[0, at].astype(F32) + direct_in[1, at].astype(F32)
        second = base[HALF:] + direct_in[0, at].astype(F32) + sum_in[1, at].astype(F32)
        return jnp.concatenate([first, second], axis=0).astype(BF)

    crossings[0].wait_recv()
    for i in range(2, 6):
        hops[0, i].wait_recv()
    for i in range(WIDE):
        y_far[:, i] = summed(0, i)
    ups = [
        send(
            y_far.at[slot], y_far_in.at[slot], ry_send.at[0, slot], ry_recv.at[0, slot],
            me.at(dy=SLOTS[slot], pair=1),
        )
        for slot in reversed(range(NY))
    ]
    for i in range(2, 6):
        hops[1, i].wait_recv()
    for i in range(NARROW):
        y_near[:, me.side + i] = summed(1, i)
    y_near[:, 4 * (1 - me.side)] = y_far[:, 4 * me.side]
    ups += [
        send(
            y_near.at[slot], y_near_in.at[slot - 1], ry_send.at[1, slot], ry_recv.at[1, slot],
            me.at(dy=SLOTS[slot]),
        )
        for slot in reversed(range(1, NY))
    ]
    for up in ups:
        up.wait_recv()
    part = y_near[0].astype(F32)
    for i in range(NY):
        part += y_far_in[i].astype(F32)
    for i in range(NY - 1):
        part += y_near_in[i].astype(F32)
    w_ref[...] = part

    order = me.zl // 2
    rotary = w_ref[4 * (1 - me.side)]
    z_out[0:2] = w_ref[pl.ds(2 + me.side, 2)].astype(BF)
    z_out[2] = jnp.concatenate([rotary[:, rope:], rotary[:, :rope]], axis=1).astype(BF)
    ups = [
        send(
            z_out, z_far.at[order], rz_send.at[2 + i], rz_recv.at[2 + i], me.at(far=1, mirror=True, dzl=2 * i)
        )
        for i in range(3)
    ]
    z_own[order, 0:2] = w_ref[pl.ds(me.side, 2)].astype(BF)
    z_own[order, 2] = rotary.astype(BF)
    ups += [
        send(
            z_own.at[order], z_own.at[order], rz_send.at[i], rz_recv.at[i], me.at(dzl=2 * i + 2)
        )
        for i in range(2)
    ]
    for up in ups:
        up.wait_recv()
    part = z_own[0].astype(F32)
    for i in range(1, 3):
        part += z_own[i].astype(F32)
    for i in range(3):
        part += z_far[i].astype(F32)
    final[me.side, me.k, me.x] = part.astype(BF)
    place = final.at[me.side, me.k, me.x]
    ups = [
        send(place, place, f_send.at[i], f_recv.at[i], me.at(**peer))
        for i, peer in enumerate(finals)
    ]
    for copy in pending[: -len(finals)]:
        copy.wait_send()
    for up in ups:
        up.wait()


def write_kernel(rope, att, qg, final, att_hbm, qg_hbm, grad_hbm, grad, sem):
    copies = [
        pltpu.make_async_copy(src, dst, sem.at[i])
        for i, (src, dst) in enumerate(((att, att_hbm), (qg, qg_hbm), (grad, grad_hbm)))
    ]
    copies[0].start()
    copies[1].start()
    width, rows = grad.shape
    for side in range(2):
        for t in range(2):
            at = (2 * side + t) * LANES
            grad[at : at + LANES, :] = final[side, :, :, t].reshape(rows, LANES).astype(F32).T
    grad[width - rope :, :] = final[0, :, :, 2].reshape(rows, LANES).astype(F32).T[:rope]
    copies[2].start()
    for copy in copies:
        copy.wait()


def on_device(queries, latent, block_of, key_up, value_up, out_grad):
    rows, joined = latent.shape
    heads, nope, width = key_up.shape
    value = value_up.shape[2]
    rope = joined - width
    scale = 1.0 / math.sqrt(nope + rope)
    both = heads * rows
    total = NZH * NX * NC * NY * SR
    vmem = pl.BlockSpec(memory_space=pltpu.VMEM)
    anywhere = pl.BlockSpec(memory_space=pl.ANY)
    dma = pltpu.SemaphoreType.DMA
    tile = (SR, LANES)
    results = pl.pallas_call(
        functools.partial(kernel, scale, nope, rope, width, value, heads),
        out_shape=(
            pltpu.VMEM(out_grad.shape, BF),
            pltpu.VMEM(queries.shape, BF),
            pltpu.VMEM((2, NC, NX, 3, *tile), BF),
        ),
        in_specs=[anywhere] * 6,
        out_specs=(vmem,) * 3,
        scratch_shapes=[
            pltpu.SMEM(block_of.shape, jnp.int32),
            pltpu.VMEM((joined, rows), BF),
            pltpu.VMEM((rows, joined), BF),
            pltpu.VMEM(queries.shape, BF),
            pltpu.VMEM(out_grad.shape, BF),
            pltpu.VMEM(key_up.shape, BF),
            pltpu.VMEM(value_up.shape, BF),
            dma((6,)),
            pltpu.VMEM((NZH, NX, NC, NY, SR, joined), BF),
            pltpu.VMEM((both, rope), BF),
            pltpu.VMEM((both, width), BF),
            pltpu.VMEM((both, width), BF),
            pltpu.VMEM((both, total), F32),
            pltpu.VMEM((both, total), F32),
            pltpu.VMEM((both, total), BF),
            pltpu.VMEM((both, total), BF),
            pltpu.VMEM((NC, NX, TILES, NY, *tile), BF),
            pltpu.VMEM((NX, TILES, NY, *tile), BF),
            pltpu.VMEM((NX - 1, TILES, NY, *tile), BF),
            pltpu.VMEM((2, TILES, HALF, *tile), BF),
            pltpu.VMEM((2, TILES, HALF, *tile), BF),
            pltpu.VMEM((2, TILES, HALF, *tile), BF),
            pltpu.VMEM((2, TILES, HALF, *tile), BF),
            pltpu.VMEM((NY, WIDE, *tile), BF),
            pltpu.VMEM((NY, WIDE, *tile), BF),
            pltpu.VMEM((NY, WIDE, *tile), BF),
            pltpu.VMEM((NY - 1, WIDE, *tile), BF),
            pltpu.VMEM((WIDE, *tile), F32),
            pltpu.VMEM((3, 3, *tile), BF),
            pltpu.VMEM((3, *tile), BF),
            pltpu.VMEM((3, 3, *tile), BF),
            dma((2, NY - 1)), dma((2, NY - 1)),
            dma, dma,
            dma((2, 12)), dma((2, 12)),
            dma((2, NX)), dma((2, NX)),
            dma((NX,)), dma((NX,)),
            dma((2, 6)), dma((2, 6)),
            dma((2, NY)), dma((2, NY)),
            dma((5,)), dma((5,)),
            dma((15,)), dma((15,)),
        ],
        compiler_params=pltpu.CompilerParams(
            collective_id=0, has_side_effects=True, vmem_limit_bytes=56 * 1024 * 1024
        ),
    )(block_of, latent.T, queries, out_grad, key_up, value_up)

    attended, query_grad, grad = pl.pallas_call(
        functools.partial(write_kernel, rope),
        out_shape=(
            jax.ShapeDtypeStruct(out_grad.shape, BF),
            jax.ShapeDtypeStruct(queries.shape, BF),
            jax.ShapeDtypeStruct((joined, rows), F32),
        ),
        in_specs=[vmem] * 3,
        out_specs=(anywhere,) * 3,
        scratch_shapes=[pltpu.VMEM((joined, rows), F32), dma((3,))],
    )(*(pltpu.with_memory_space_constraint(a, pltpu.VMEM) for a in results))
    return attended, query_grad, grad.T


def solution(mesh):
    return jax.shard_map(
        on_device,
        mesh=mesh,
        in_specs=(
            P("ctx", "head"),
            P("ctx", None),
            P(),
            P("head", None, None),
            P("head", None, None),
            P("ctx", "head"),
        ),
        out_specs=(P("ctx", "head"), P("ctx", "head"), P("ctx", None)),
        check_vma=False,
    )
```
